32 devices in a mesh: row: 4 (over y, x), col: 4 (over z), head: 2 (over core).
Axes of the slice: x: 2, y: 2, z: 4, core: 2. Of those that a mesh axis runs over, the one named last changes fastest.
Arguments:
- queries: bfloat16 [256, 64, 256], P('row', 'col'), may hold values from -1000 to 1000
- level_zero: bfloat16 [256, 64, 256], P('row', 'col', 'head'), may hold values from -6 to 6
- level_one: bfloat16 [128, 32, 256], P('row', 'col', 'head'), may hold values from -6 to 6
- level_two: bfloat16 [64, 16, 256], P('row', 'col', 'head'), may hold values from -6 to 6
- level_three: bfloat16 [32, 8, 256], P('row', 'col', 'head'), may hold values from -6 to 6
- tile_lists: int32 [16, 4, 4, 8], P('row', 'col'), may hold values from 0 to 63, as said below
- samples: int32 [256, 64, 128], P('row', 'col', 'head'), may hold values from 0 to 133168895, as said below
- logit_weight: bfloat16 [256, 128], P(None, 'head'), may hold values from -1 to 1
- logit_bias: float32 [128], P('head'), may hold values from -3 to 3
- output_weight: bfloat16 [256, 256], replicated, may hold values from -0.375 to 0.375
- output_bias: float32 [256], replicated, may hold values from -3 to 3
- norm_gain: float32 [256], P('head'), may hold values from 0.5 to 1.5
- norm_shift: float32 [256], P('head'), may hold values from -3 to 3
Outputs:
- updated_queries: bfloat16 [256, 64, 256], P('row', 'col', 'head')
The draws below stay inside these ranges and needn't reach their ends.
Inputs may be any that keep to these rules, and one draw needn't show every extreme that they name: `tile_lists`: entries are tile numbers r * 4 + c. Over all lists of the query blocks that one device holds, at one level, at most 2 entries name tiles that one device holds; at each level some device is named exactly 2 times by the lists of every device. A tile may be listed more than once. `samples`: slot is below 8; at level l, pos_row and pos_col are below (16 / 2^l - 1) * 256.
All inputs are finite; a program needn't handle non-finite values.
Results may differ from the reference program's by a relative error of at most 0.004.
Values may be sent and summed in bfloat16 or wider, within the bound.
A program may use at most 128 MiB of HBM per device.

```python
import math
import jax
import jax.numpy as jnp
from jax import lax

D = 256
HEADS = 8
LEVELS = 4
POINTS = 4
TILE = 16
K = 8
TR = 4
TC = 1
ROWS = 256
COLS = 64
N_ROW = 4
N_COL = 4


def attend_columns(key):
    raw_draw = jax.random.normal(jax.random.fold_in(key, 701), (D, HEADS * LEVELS * POINTS), jnp.float32)
    return (jnp.clip(raw_draw, -5.0, 5.0) / math.sqrt(D)).astype(jnp.bfloat16)


def draw_logit_weight(key, part):
    return attend_columns(key)


def draw_queries(key, part):
    height = TR * TILE * N_ROW
    width_all = TC * TILE * N_COL
    base_draw = jax.random.normal(jax.random.fold_in(key, 1), (height, width_all, D), jnp.float32)
    base_draw = jnp.clip(base_draw, -6.0, 6.0)
    return base_draw.astype(jnp.bfloat16)


def draw_samples(key, part):
    height = TR * TILE * N_ROW
    width_all = TC * TILE * N_COL
    lane_count = HEADS * LEVELS * POINTS
    lane_level = jnp.arange(lane_count, dtype=jnp.int32) // POINTS % LEVELS
    pos_limit = (TILE // jnp.left_shift(jnp.int32(1), lane_level) - 1) * 256
    full_shape = (height, width_all, lane_count)
    slot_draw = jax.random.randint(jax.random.fold_in(key, 21), full_shape, 0, K)
    row_draw = jax.random.randint(jax.random.fold_in(key, 22), full_shape, 0, jnp.broadcast_to(pos_limit, full_shape))
    col_draw = jax.random.randint(jax.random.fold_in(key, 23), full_shape, 0, jnp.broadcast_to(pos_limit, full_shape))
    return (slot_draw * 16777216 + row_draw * 4096 + col_draw).astype(jnp.int32)


def draw_tile_lists(key, part):
    peer_count = N_ROW * N_COL
    local_tiles = TR * TC
    requests = local_tiles * K
    capacity = max(2, (requests + peer_count - 1) // peer_count)
    slot_count = peer_count * capacity
    hot_owner = jax.random.randint(jax.random.fold_in(key, 31), (LEVELS,), 0, peer_count)

    def one_list(device_num, level_num):
        sub_key = jax.random.fold_in(jax.random.fold_in(key, 32), device_num * LEVELS + level_num)
        scores = jax.random.permutation(jax.random.fold_in(sub_key, 1), slot_count).astype(jnp.int32)
        forced = jnp.arange(slot_count, dtype=jnp.int32) // capacity == hot_owner[level_num]
        scores = jnp.where(forced, -1, scores)
        ranking = jnp.argsort(scores, stable=True)
        chosen = ranking[:requests]
        chosen = chosen[jax.random.permutation(jax.random.fold_in(sub_key, 2), requests)]
        owner_dev = chosen.astype(jnp.int32) // capacity
        local_index = jax.random.randint(jax.random.fold_in(sub_key, 3), (requests,), 0, local_tiles)
        tile_row = owner_dev // N_COL * TR + local_index // TC
        tile_col = owner_dev % N_COL * TC + local_index % TC
        return (tile_row * (TC * N_COL) + tile_col).astype(jnp.int32)
    device_grid = jnp.arange(peer_count, dtype=jnp.int32)
    level_grid = jnp.arange(LEVELS, dtype=jnp.int32)
    tile_ids = jax.vmap(lambda device_num: jax.vmap(lambda level_num: one_list(device_num, level_num))(level_grid))(device_grid)
    tile_ids = tile_ids.reshape(N_ROW, N_COL, LEVELS, TR, TC, K)
    return tile_ids.transpose(0, 3, 1, 4, 2, 5).reshape(TR * N_ROW, TC * N_COL, LEVELS, K)


def levels(rng, dims, split, least, largest):
    gain = 1.0
    for position, shards_of in split:
        heights = jax.random.uniform(jax.random.fold_in(jax.random.fold_in(rng, 6), position), (shards_of,), jnp.float32, least / len(split), largest / len(split))
        gain = gain * jnp.repeat(jnp.exp(heights), dims[position] // shards_of).reshape((-1,) + (1,) * (len(dims) - 1 - position))
    return gain


def scatter_about(key, shape, deviation, most, cuts=(), kind=jnp.bfloat16):
    values = jax.random.normal(key, shape, jnp.float32) * deviation
    if len(cuts) > 0:
        values = levels(key, shape, cuts, -0.22, 0.18) * values
    return jnp.clip(values, min=-most, max=most).astype(kind)


def setup_inputs(seed: int = 0) -> dict:
    key_list = jax.random.split(jax.random.key(seed), 14)
    queries = draw_queries(jax.random.fold_in(key_list[13], 71), 0)
    level_zero = scatter_about(key_list[1], (ROWS, COLS, D), 1.0, 6.0, ((0, 4), (1, 4), (2, 2)))
    level_one = scatter_about(key_list[2], (ROWS // 2, COLS // 2, D), 1.0, 6.0, ((0, 4), (1, 4), (2, 2)))
    level_two = scatter_about(key_list[3], (ROWS // 4, COLS // 4, D), 1.0, 6.0, ((0, 4), (1, 4), (2, 2)))
    level_three = scatter_about(key_list[4], (ROWS // 8, COLS // 8, D), 1.0, 6.0, ((0, 4), (1, 4), (2, 2)))
    tile_lists = draw_tile_lists(jax.random.fold_in(key_list[13], 71), 0)
    samples = draw_samples(jax.random.fold_in(key_list[13], 71), 0)
    logit_weight = draw_logit_weight(jax.random.fold_in(key_list[13], 71), 0)
    logit_bias = scatter_about(key_list[8], (HEADS * LEVELS * POINTS,), 0.5, 3.0, ((0, 2),), jnp.float32)
    output_weight = scatter_about(key_list[9], (D, D), D ** -0.5, 0.375)
    output_bias = scatter_about(key_list[10], (D,), 0.5, 3.0, (), jnp.float32)
    norm_gain = jnp.clip(1.0 + 0.1 * jax.random.normal(key_list[11], (D,), jnp.float32), 0.5, 1.5)
    norm_shift = scatter_about(key_list[12], (D,), 0.5, 3.0, ((0, 2),), jnp.float32)
    return dict(queries=queries, level_zero=level_zero, level_one=level_one, level_two=level_two, level_three=level_three, tile_lists=tile_lists, samples=samples, logit_weight=logit_weight, logit_bias=logit_bias, output_weight=output_weight, output_bias=output_bias, norm_gain=norm_gain, norm_shift=norm_shift)


def to_blocks(source, grid_rows, grid_cols, tile_side):
    channels = source.shape[2]
    shaped = source.reshape(grid_rows, tile_side, grid_cols, tile_side, channels)
    return shaped.transpose(0, 2, 1, 3, 4).reshape(grid_rows * grid_cols, tile_side * tile_side, channels)

def reference(queries, level_zero, level_one, level_two, level_three, tile_lists, samples, logit_weight, logit_bias, output_weight, output_bias, norm_gain, norm_shift):
    grid_rows = tile_lists.shape[0]
    grid_cols = tile_lists.shape[1]
    head_dim = D // HEADS
    pixels = TILE * TILE
    hits = POINTS * 4
    tile_sets = []
    for level_num, level_array in enumerate((level_zero, level_one, level_two, level_three)):
        tile_side = TILE // 2 ** level_num
        blocks_here = to_blocks(level_array, grid_rows, grid_cols, tile_side)
        tile_sets.append(blocks_here.reshape(grid_rows * grid_cols, tile_side * tile_side, HEADS, head_dim))
    query_blocks = to_blocks(queries, grid_rows, grid_cols, TILE)
    sample_blocks = to_blocks(samples, grid_rows, grid_cols, TILE)
    list_blocks = tile_lists.reshape(grid_rows * grid_cols, LEVELS, K)
    earlier = jnp.arange(hits, dtype=jnp.int32)[None, :] < jnp.arange(hits, dtype=jnp.int32)[:, None]

    def one_block(operands):
        query_blk, sample_blk, list_blk = operands
        logits = jnp.dot(query_blk, logit_weight, preferred_element_type=jnp.float32) + logit_bias
        attend = jax.nn.softmax(logits.reshape(pixels, HEADS, LEVELS * POINTS), axis=-1)
        attend = attend.reshape(pixels, HEADS, LEVELS, POINTS)
        packed = sample_blk.reshape(pixels, HEADS, LEVELS, POINTS)
        slot_index = packed // 16777216
        pos_row = packed // 4096 % 4096
        pos_col = packed % 4096
        frac_row = (pos_row % 256).astype(jnp.float32) / 256.0
        frac_col = (pos_col % 256).astype(jnp.float32) / 256.0
        running = jnp.zeros((pixels, HEADS, head_dim), jnp.float32)
        for level_num in range(LEVELS):
            tile_side = TILE // 2 ** level_num
            chosen = tile_sets[level_num][list_blk[level_num]]
            flat_values = chosen.reshape(K * tile_side * tile_side, HEADS, head_dim).transpose(1, 0, 2)
            base_index = slot_index[:, :, level_num] * tile_side * tile_side + pos_row[:, :, level_num] // 256 * tile_side + pos_col[:, :, level_num] // 256
            lvl_row = frac_row[:, :, level_num]
            lvl_col = frac_col[:, :, level_num]
            attend_lvl = attend[:, :, level_num]
            targets = jnp.stack([base_index, base_index + 1, base_index + tile_side, base_index + tile_side + 1], axis=3).reshape(pixels, HEADS, hits)
            corner_weights = jnp.stack([attend_lvl * (1.0 - lvl_row) * (1.0 - lvl_col), attend_lvl * (1.0 - lvl_row) * lvl_col, attend_lvl * lvl_row * (1.0 - lvl_col), attend_lvl * lvl_row * lvl_col], axis=3).reshape(pixels, HEADS, hits)
            same_pixel = targets[:, :, :, None] == targets[:, :, None, :]
            combined = lax.optimization_barrier(jnp.sum(jnp.where(same_pixel, corner_weights[:, :, None, :], 0.0), axis=3))
            repeated = jnp.any(same_pixel & earlier, axis=3)
            rounded = lax.optimization_barrier(combined.astype(jnp.bfloat16)).astype(jnp.float32)
            pixel_weight = jnp.where(repeated, 0.0, rounded)
            lookup = targets.transpose(1, 0, 2).reshape(HEADS, pixels * hits)
            picked = jnp.take_along_axis(flat_values, lookup[:, :, None], axis=1).astype(jnp.float32)
            picked = picked.reshape(HEADS, pixels, hits, head_dim)
            running = running + jnp.einsum('qhn,hqnd->qhd', pixel_weight, picked, precision=lax.Precision.HIGHEST)
        attn_out = running.reshape(pixels, D).astype(jnp.bfloat16)
        pre_norm = query_blk.astype(jnp.float32) + jnp.dot(attn_out, output_weight, preferred_element_type=jnp.float32) + output_bias
        row_mean = lax.optimization_barrier(jnp.mean(pre_norm, axis=1, keepdims=True))
        centered = pre_norm - row_mean
        variance = lax.optimization_barrier(jnp.mean(centered * centered, axis=1, keepdims=True))
        return (centered * lax.rsqrt(variance + 1e-05) * norm_gain + norm_shift).astype(jnp.bfloat16)
    updated = lax.map(one_block, (query_blocks, sample_blocks, list_blocks))
    updated = updated.reshape(grid_rows, grid_cols, TILE, TILE, D).transpose(0, 2, 1, 3, 4)
    return updated.reshape(grid_rows * TILE, grid_cols * TILE, D)
```

```python
import functools

import jax
import jax.numpy as jnp
from jax import lax
from jax.experimental import pallas as pl
from jax.experimental.pallas import tpu as pltpu
from jax.sharding import PartitionSpec as P

LEVELS = 4
POINTS = 4
PACK = 16
MESH = pl.DeviceIdType.MESH


def to_blocks(source, tile_rows, tile_cols, tile_side):
    channels = source.shape[2]
    shaped = source.reshape(tile_rows, tile_side, tile_cols, tile_side, channels)
    return shaped.transpose(0, 2, 1, 3, 4).reshape(
        tile_rows * tile_cols, tile_side * tile_side, channels
    )


def hat(index, start, low, high):
    return jnp.where(index == start, low, jnp.where(index == start + 1, high, 0.0))


def prepare(head_count, b, query_ref, lw_ref, lb_ref, samples_ref, point_s, corner_s):
    queries_here = query_ref.shape[1]
    hits = LEVELS * POINTS
    logits = lax.dot_general(
        lw_ref[...], query_ref[b], (((1,), (1,)), ((), ())), preferred_element_type=jnp.float32
    ) + lb_ref[...]
    logits = logits.reshape(head_count, hits, queries_here)
    shifted = jnp.exp(logits - jnp.max(logits, axis=1, keepdims=True))
    attend = shifted / jnp.sum(shifted, axis=1, keepdims=True)
    attend = attend.reshape(head_count * hits, queries_here)
    packed = samples_ref[b].T
    pos_row = (packed >> 12) & 4095
    pos_col = packed & 4095
    frac_row = (pos_row & 255).astype(jnp.float32) * (1.0 / 256.0)
    frac_col = (pos_col & 255).astype(jnp.float32) * (1.0 / 256.0)
    point_s[b, 0] = packed >> 24
    point_s[b, 1] = pos_row >> 8
    point_s[b, 2] = pos_col >> 8
    corner_s[b, 0] = attend * (1.0 - frac_row)
    corner_s[b, 1] = attend * frac_row
    corner_s[b, 2] = 1.0 - frac_col
    corner_s[b, 3] = frac_col


def weigh(sides, spans, per_block, b, h, slab, point_s, corner_s, mask_s, weight_s):
    hits = LEVELS * POINTS
    queries_here = weight_s.shape[2]
    lane_row = lax.broadcasted_iota(jnp.int32, (PACK, queries_here), 0)
    slot_row = lax.broadcasted_iota(jnp.int32, (per_block, queries_here), 0)
    level_off = 0
    for level_num in range(LEVELS):
        side = sides[level_num]
        span = spans[level_num]
        rows = [pl.ds(h * hits + level_num * POINTS + p, 1) for p in range(POINTS)]
        for p in range(POINTS):
            mask_s[p * per_block:(p + 1) * per_block, :] = jnp.where(
                slot_row == point_s[b, 0, rows[p], :], 1.0, 0.0
            )
        cols = [
            hat(lane_row % side, point_s[b, 2, rows[p], :], corner_s[b, 2, rows[p], :],
                corner_s[b, 3, rows[p], :])
            for p in range(POINTS)
        ]
        rows_per_chunk = PACK // side

        def chunk(step, carry, rows=rows, cols=cols, side=side, span=span,
                  level_off=level_off, rows_per_chunk=rows_per_chunk):
            parts = []
            for p in range(POINTS):
                index = step * rows_per_chunk
                start = point_s[b, 1, rows[p], :]
                low = corner_s[b, 0, rows[p], :]
                high = corner_s[b, 1, rows[p], :]
                if rows_per_chunk > 1:
                    across = hat(index + lane_row // side, start, low, high)
                else:
                    across = jnp.where(
                        start == index, low, jnp.where(start == index - 1, high, 0.0)
                    )
                parts.append(cols[p] * across)
            for k in range(per_block):
                total = parts[0] * mask_s[k:k + 1, :]
                for p in range(1, POINTS):
                    total = total + parts[p] * mask_s[p * per_block + k:p * per_block + k + 1, :]
                where = pl.multiple_of(level_off + k * span + step * PACK, PACK)
                weight_s[slab, pl.ds(where, PACK), :] = total.astype(jnp.bfloat16)
            return carry

        chunks = span // PACK
        if chunks == 1:
            chunk(0, 0)
        else:
            lax.fori_loop(0, chunks, chunk, 0)
        level_off += span * per_block


def exchange_kernel(sides, spans, per_block, head_count, rows, cols, capacity, local_tiles, *refs):
    (table_ref, tiles_ref, query_ref, lw_ref, lb_ref, samples_ref, fetched_ref, weights_ref) = refs[:8]
    refs = refs[8:]
    held = refs[:cols - 1]
    (ids_v, stage, point_s, corner_s, mask_s, weight_s, id_send, id_recv, col_send, col_recv,
     row_send, row_recv, own_sem, ids_sem, weight_sem) = refs[cols - 1:]
    r = lax.axis_index("row")
    c = lax.axis_index("col")
    lanes_wide = tiles_ref.shape[1]
    barrier = pltpu.get_barrier_semaphore()
    for dc in range(1, cols):
        pl.semaphore_signal(barrier, inc=1, device_id={"col": lax.rem(c + dc, cols)}, device_id_type=MESH)
    for dr in range(1, rows):
        pl.semaphore_signal(barrier, inc=1, device_id={"row": lax.rem(r + dr, rows)}, device_id_type=MESH)
    pl.semaphore_wait(barrier, cols + rows - 2)

    id_copies = []
    for dr in range(1, rows):
        to = lax.rem(r + dr, rows)
        copy = pltpu.make_async_remote_copy(
            table_ref.at[to], ids_v.at[dr], id_send.at[dr], id_recv.at[dr],
            device_id={"row": to}, device_id_type=MESH,
        )
        copy.start()
        id_copies.append(copy)
    col_copies = []
    for dc in range(1, cols):
        copy = pltpu.make_async_remote_copy(
            tiles_ref, held[dc - 1], col_send.at[dc], col_recv.at[dc],
            device_id={"col": lax.rem(c + dc, cols)}, device_id_type=MESH,
        )
        copy.start()
        col_copies.append(copy)
    own_ids = pltpu.make_async_copy(table_ref.at[r], ids_v.at[0], ids_sem)
    own_ids.start()
    own_ids.wait()
    for copy in id_copies:
        copy.wait()

    def pick(dc):
        owner_col = lax.rem(c - dc + cols, cols)
        source = tiles_ref if dc == 0 else held[dc - 1]
        out_at = (r * cols + owner_col) * capacity
        copies = []
        for turn in range(rows):
            dr = (turn + 1) % rows
            for place in range(capacity):
                off = 0
                for level_num in range(LEVELS):
                    span = spans[level_num]
                    at = (owner_col * capacity + place) * LEVELS + level_num
                    asked = jnp.broadcast_to(ids_v[dr, pl.ds(at, 1), :], (PACK, lanes_wide))
                    shape = (span // PACK, PACK, lanes_wide)
                    total = None
                    for tile in range(local_tiles):
                        mask = jnp.where(asked == tile, 1.0, 0.0).astype(jnp.bfloat16)
                        first = local_tiles * off + tile * span
                        part = source[first:first + span, :].reshape(shape) * mask[None]
                        total = part if total is None else total + part
                    stage[dr, dc, place, off:off + span, :] = total.reshape(span, lanes_wide)
                    off += span
            target = fetched_ref.at[pl.ds(out_at, capacity)]
            if dr == 0:
                copy = pltpu.make_async_copy(stage.at[dr, dc], target, own_sem.at[dc])
            else:
                copy = pltpu.make_async_remote_copy(
                    stage.at[dr, dc], target, row_send.at[dr, dc], row_recv.at[dr, dc],
                    device_id={"row": lax.rem(r - dr + rows, rows)}, device_id_type=MESH,
                )
            copy.start()
            copies.append(copy)
        return copies

    copies = pick(0)

    def prepare_one(b, carry):
        prepare(head_count, b, query_ref, lw_ref, lb_ref, samples_ref, point_s, corner_s)
        return carry

    lax.fori_loop(0, local_tiles, prepare_one, 0)

    def store(step, slab):
        return pltpu.make_async_copy(
            weight_s.at[slab], weights_ref.at[step // head_count, step % head_count],
            weight_sem.at[slab],
        )

    def weigh_one(step, carry):
        slab = step % 2

        @pl.when(step >= 2)
        def _():
            store(step - 2, slab).wait()

        weigh(sides, spans, per_block, step // head_count, step % head_count, slab,
              point_s, corner_s, mask_s, weight_s)
        store(step, slab).start()
        return carry

    steps = local_tiles * head_count
    done = 0
    for dc in range(1, cols):
        until = steps * dc // (cols - 1)
        if until > done:
            lax.fori_loop(done, until, weigh_one, 0)
        done = until
        col_copies[dc - 1].wait()
        copies += pick(dc)
    for step in range(max(0, steps - 2), steps):
        store(step, step % 2).wait()
    for copy in copies:
        copy.wait()


def mix_kernel(spans, per_block, head_count, head_dim, pos_ref, fetched_ref, upper_ref, lower_ref,
               out_ref,
               values, values_t, mixed, sem):
    block = pl.program_id(0)
    h = pl.program_id(1)
    blocks = pl.num_programs(0)

    def fetch(which):
        off = 0
        src = 0
        for level_num in range(LEVELS):
            span = spans[level_num]
            for k in range(per_block):
                pltpu.make_async_copy(
                    fetched_ref.at[pos_ref[level_num, which * per_block + k], pl.ds(src, span), :],
                    values.at[which % 2, pl.ds(off, span), :],
                    sem.at[which % 2],
                ).start()
                off += span
            src += span

    @pl.when((h == 0) & (block == 0))
    def _():
        fetch(block)

    @pl.when(h == 0)
    def _():
        side = block % 2
        pltpu.make_async_copy(values.at[side], values.at[side], sem.at[side]).wait()
        values_t[...] = values[side].T.reshape(values_t.shape)

        @pl.when(block + 1 < blocks)
        def _():
            fetch(block + 1)

    half = upper_ref.shape[2]
    mixed[h] = jnp.dot(
        values_t[h, :, :half], upper_ref[0, 0], preferred_element_type=jnp.float32
    ) + jnp.dot(values_t[h, :, half:], lower_ref[0, 0], preferred_element_type=jnp.float32)

    @pl.when(h == head_count - 1)
    def _():
        whole = mixed[...].reshape(head_count * head_dim, mixed.shape[2])
        out_ref[...] = whole.T.astype(jnp.bfloat16)


def gathered_attention(queries, level_blocks, tile_lists, samples, logit_weight, logit_bias, sides, spans):
    row_count = lax.axis_size("row")
    col_count = lax.axis_size("col")
    peer_count = row_count * col_count
    tile_rows, tile_cols, level_count, per_block = tile_lists.shape
    local_tiles = tile_rows * tile_cols
    requests = local_tiles * per_block
    capacity = max(2, (requests + peer_count - 1) // peer_count)
    slots = peer_count * capacity
    grid_cols = tile_cols * col_count
    channels = level_blocks[0].shape[2]
    head_count = samples.shape[2] // (LEVELS * POINTS)
    head_dim = channels // head_count
    tile_side = sides[0]
    pixels = tile_side * tile_side
    tile_span = sum(spans)
    depth = per_block * tile_span

    wanted = tile_lists.transpose(2, 0, 1, 3).reshape(level_count, requests)
    grid_row = wanted // grid_cols
    grid_col = wanted % grid_cols
    owner_dev = grid_row // tile_rows * col_count + grid_col // tile_cols
    local_index = grid_row % tile_rows * tile_cols + grid_col % tile_cols
    order = jnp.arange(requests, dtype=jnp.int32)
    earlier = (owner_dev[:, :, None] == owner_dev[:, None, :]) & (order[None, :] < order[:, None])
    positions = owner_dev * capacity + jnp.sum(earlier.astype(jnp.int32), axis=2)
    slot_order = jnp.arange(slots, dtype=jnp.int32)
    named = positions[:, None, :] == slot_order[None, :, None]
    slot_table = jnp.max(jnp.where(named, local_index[:, None, :], -1), axis=2)
    table = jnp.maximum(slot_table, 0).reshape(level_count, row_count, col_count * capacity)
    table = table.transpose(1, 2, 0).reshape(row_count, col_count * capacity * level_count, 1)
    table_rows = table.shape[1]
    table = jnp.broadcast_to(table, (row_count, table_rows, channels))

    tiles_local = []
    for level_num in range(level_count):
        tiles = to_blocks(level_blocks[level_num], tile_rows, tile_cols, sides[level_num])
        short = spans[level_num] - tiles.shape[1]
        if short > 0:
            tiles = jnp.pad(tiles, ((0, 0), (0, short), (0, 0)))
        tiles_local.append(tiles.reshape(local_tiles * spans[level_num], channels))
    tiles_local = jnp.concatenate(tiles_local, axis=0)

    queries_blocked = to_blocks(queries, tile_rows, tile_cols, tile_side)
    samples_blocked = to_blocks(samples, tile_rows, tile_cols, tile_side)
    lanes = head_count * LEVELS * POINTS
    vmem = pl.BlockSpec(memory_space=pltpu.VMEM)
    whole = pl.BlockSpec(memory_space=pl.ANY)
    dma = pltpu.SemaphoreType.DMA
    fetched, weights = pl.pallas_call(
        functools.partial(exchange_kernel, sides, spans, per_block, head_count, row_count,
                          col_count, capacity, local_tiles),
        out_shape=(
            jax.ShapeDtypeStruct((slots, tile_span, channels), jnp.bfloat16),
            jax.ShapeDtypeStruct((local_tiles, head_count, depth, pixels), jnp.bfloat16),
        ),
        in_specs=[vmem] * 6,
        out_specs=(whole, whole),
        scratch_shapes=[
            pltpu.VMEM((local_tiles * tile_span, channels), jnp.bfloat16)
            for _ in range(col_count - 1)
        ] + [
            pltpu.VMEM((row_count, table_rows, channels), jnp.int32),
            pltpu.VMEM((row_count, col_count, capacity, tile_span, channels), jnp.bfloat16),
            pltpu.VMEM((local_tiles, 3, lanes, pixels), jnp.int32),
            pltpu.VMEM((local_tiles, 4, lanes, pixels), jnp.float32),
            pltpu.VMEM((POINTS * per_block, pixels), jnp.float32),
            pltpu.VMEM((2, depth, pixels), jnp.bfloat16),
            dma((row_count,)), dma((row_count,)), dma((col_count,)), dma((col_count,)),
            dma((row_count, col_count)), dma((row_count, col_count)), dma((col_count,)),
            dma, dma((2,)),
        ],
        compiler_params=pltpu.CompilerParams(
            collective_id=0, has_side_effects=True, vmem_limit_bytes=60 * 1024 * 1024
        ),
        cost_estimate=pl.CostEstimate(
            flops=8 * local_tiles * head_count * depth * pixels * POINTS,
            bytes_accessed=2 * local_tiles * head_count * depth * pixels, transcendentals=0,
        ),
        name="exchange",
    )(table, tiles_local, queries_blocked, logit_weight.T, logit_bias[:, None], samples_blocked)

    attn_out = pl.pallas_call(
        functools.partial(mix_kernel, spans, per_block, head_count, head_dim),
        grid_spec=pltpu.PrefetchScalarGridSpec(
            num_scalar_prefetch=1,
            grid=(local_tiles, head_count),
            in_specs=[
                pl.BlockSpec(memory_space=pl.ANY),
                pl.BlockSpec((1, 1, depth // 2, pixels), lambda b, h, pos: (b, h, 0, 0)),
                pl.BlockSpec((1, 1, depth // 2, pixels), lambda b, h, pos: (b, h, 1, 0)),
            ],
            out_specs=pl.BlockSpec((pixels, channels), lambda b, h, pos: (b, 0)),
            scratch_shapes=[
                pltpu.VMEM((2, depth, channels), jnp.bfloat16),
                pltpu.VMEM((head_count, head_dim, depth), jnp.bfloat16),
                pltpu.VMEM((head_count, head_dim, pixels), jnp.float32),
                pltpu.SemaphoreType.DMA((2,)),
            ],
        ),
        out_shape=jax.ShapeDtypeStruct((local_tiles * pixels, channels), jnp.bfloat16),
        compiler_params=pltpu.CompilerParams(
            dimension_semantics=("arbitrary", "arbitrary"), vmem_limit_bytes=60 * 1024 * 1024
        ),
        cost_estimate=pl.CostEstimate(
            flops=2 * local_tiles * depth * pixels * channels,
            bytes_accessed=2 * local_tiles * head_count * depth * pixels, transcendentals=0,
        ),
        name="mix",
    )(positions, fetched, weights, weights)
    return attn_out


def power_of_two(n):
    return n > 0 and n & (n - 1) == 0


def group_order(c, cols):
    near = jnp.minimum(c, cols - 1 - c)
    order = [c]
    for g in range(1, cols):
        both = c - (g + 1) // 2 if g % 2 else c + g // 2
        one = jnp.where(c < cols - 1 - c, c + g - near, c - g + near)
        order.append(jnp.where(g <= 2 * near, both, one))
    return order


def plan_tables(rows, cols, per_block, lists_ref, table, index_v):
    blocks = lists_ref.shape[0]
    wanted = jnp.concatenate([lists_ref[b] for b in range(blocks)], axis=1)
    requests = wanted.shape[1]
    tile_rows = blocks
    col_bits = cols.bit_length() - 1
    row_bits = tile_rows.bit_length() - 1
    shape = (requests, requests)
    down = lax.broadcasted_iota(jnp.int32, shape, 0)
    along = lax.broadcasted_iota(jnp.int32, shape, 1)
    capacity = requests // (rows * cols)
    for level_num in range(LEVELS):
        here = jnp.broadcast_to(wanted[level_num:level_num + 1, :], shape)
        own_here = ((here >> (col_bits + row_bits)) << col_bits) + (here & (cols - 1))
        local_here = (here >> col_bits) & (tile_rows - 1)
        same = own_here == own_here.T
        place_here = jnp.sum(jnp.where(same & (down < along), 1, 0), axis=0, keepdims=True)
        slot_here = own_here * capacity + place_here
        asked = jnp.sum(
            jnp.where(slot_here == down, local_here.astype(jnp.float32), 0.0), axis=1, keepdims=True
        )
        asked = jnp.broadcast_to(asked, (requests, table.shape[3])).astype(jnp.int32)
        table[:, level_num] = asked.reshape(rows, requests // rows, table.shape[3])
        filled = jnp.sum(jnp.where(slot_here.T == along, down, 0), axis=0, keepdims=True)
        index_v[level_num:level_num + 1, 0:requests] = filled


def points(head_count, b, query_ref, lw_ref, bias, samples_ref, point_s, corner_s, slot_s):
    queries_here = query_ref.shape[1]
    hits = LEVELS * POINTS
    logits = lax.dot_general(
        lw_ref[...], query_ref[b], (((1,), (1,)), ((), ())), preferred_element_type=jnp.float32
    ) + bias
    logits = logits.reshape(head_count, hits, queries_here)
    shifted = jnp.exp(logits - jnp.max(logits, axis=1, keepdims=True))
    attend = shifted / jnp.sum(shifted, axis=1, keepdims=True)
    attend = attend.reshape(head_count * hits, queries_here)
    packed = samples_ref[b].T
    pos_row = (packed >> 12) & 4095
    pos_col = packed & 4095
    frac_row = (pos_row & 255).astype(jnp.float32) * (1.0 / 256.0)
    frac_col = (pos_col & 255).astype(jnp.float32) * (1.0 / 256.0)
    point_s[b, 0] = pos_row >> 8
    point_s[b, 1] = pos_col >> 8
    corner_s[b, 0] = attend * (1.0 - frac_row)
    corner_s[b, 1] = attend * frac_row
    corner_s[b, 2] = 1.0 - frac_col
    corner_s[b, 3] = frac_col
    slot_s[b] = (packed >> 24).astype(jnp.float32)


def spread(sides, spans, head_count, step, point_s, corner_s, spread_s):
    hits = LEVELS * POINTS
    queries_here = spread_s.shape[3]
    b = step // head_count
    h = step % head_count
    half = PACK // 2
    lane_row = lax.broadcasted_iota(jnp.int32, (PACK, queries_here), 0)
    off = 0
    for level_num in range(LEVELS):
        side = sides[level_num]
        span = spans[level_num]
        for p in range(POINTS):
            row = pl.ds(h * hits + level_num * POINTS + p, 1)
            across = hat(lane_row % side, point_s[b, 1, row, :], corner_s[b, 2, row, :],
                         corner_s[b, 3, row, :])
            if side >= half:
                wide = (half, queries_here)
                start = jnp.broadcast_to(point_s[b, 0, row, :], wide)
                low = jnp.broadcast_to(corner_s[b, 0, row, :], wide)
                high = jnp.broadcast_to(corner_s[b, 1, row, :], wide)
                downs = [hat(i, start, low, high) for i in range(side)]
                for chunk in range(span // PACK):
                    parts = []
                    for part in range(2):
                        at = chunk * PACK + part * half
                        col = at % side
                        if side == half:
                            piece = across[part * half:(part + 1) * half, :]
                        else:
                            piece = across[col:col + half, :]
                        parts.append(piece * downs[at // side])
                    total = jnp.concatenate(parts, axis=0).astype(jnp.bfloat16)
                    spread_s[step, p, off + chunk * PACK:off + (chunk + 1) * PACK, :] = total
            else:
                down = hat(lane_row // side, point_s[b, 0, row, :], corner_s[b, 0, row, :],
                           corner_s[b, 1, row, :])
                spread_s[step, p, off:off + PACK, :] = (across * down).astype(jnp.bfloat16)
        off += span


def weigh_slots(spans, per_block, head_count, rows, cols, group, index_s, slot_s, spread_s, weight_s):
    hits = LEVELS * POINTS
    queries_here = weight_s.shape[3]
    capacity = 2
    units = rows * capacity
    block_bits = per_block.bit_length() - 1
    requests = slot_s.shape[0] * per_block

    def one(step, carry):
        h = step // units
        unit = step % units
        slot = (unit // capacity * cols + group) * capacity + unit % capacity
        off = 0
        for level_num in range(LEVELS):
            span = spans[level_num]
            entry = index_s[level_num, slot] & (requests - 1)
            b = entry >> block_bits
            k = (entry & (per_block - 1)).astype(jnp.float32)
            masks = []
            for p in range(POINTS):
                mine = slot_s[b, pl.ds(h * hits + level_num * POINTS + p, 1), :]
                mine = jnp.broadcast_to(mine, (PACK, queries_here))
                masks.append(jnp.where(mine == k, 1.0, 0.0).astype(jnp.bfloat16))
            source = b * head_count + h
            for chunk in range(span // PACK):
                total = None
                for p in range(POINTS):
                    part = masks[p] * spread_s[source, p, off + chunk * PACK:off + (chunk + 1) * PACK, :]
                    total = part if total is None else total + part
                where = pl.multiple_of(units * off + unit * span + chunk * PACK, PACK)
                weight_s[group, h, pl.ds(where, PACK), :] = total
            off += span
        return carry

    lax.fori_loop(0, head_count * units, one, 0)


def mix_slots(spans, per_block, head_count, head_dim, rows, cols, blocks, group, index_s, fetched,
              turned, weight_s, mixed):
    capacity = 2
    units = rows * capacity
    lanes = 128
    block_bits = per_block.bit_length() - 1
    turned[...] = fetched[group].T
    lane = lax.broadcasted_iota(jnp.int32, (1, lanes), 1)
    owners = []
    off = 0
    for level_num in range(LEVELS):
        span = spans[level_num]
        block_of = []
        for unit in range(units):
            slot = (unit // capacity * cols + group) * capacity + unit % capacity
            block_of.append(index_s[level_num, slot] >> block_bits)
        for start in range(0, units * span, lanes):
            first = start // span
            last = (start + lanes - 1) // span
            value = jnp.full((1, lanes), block_of[first], jnp.int32)
            for unit in range(first + 1, last + 1):
                value = jnp.where(lane >= unit * span - start, block_of[unit], value)
            owners.append(value)
        off += span
    owner_row = jnp.concatenate(owners, axis=1)
    keep = [
        jnp.broadcast_to(jnp.where(owner_row == b, 1.0, 0.0), (PACK, owner_row.shape[1])).astype(jnp.bfloat16)
        for b in range(blocks)
    ]
    keep = [jnp.concatenate([one] * (head_dim // PACK), axis=0) for one in keep]

    def one_head(h, carry):
        base = turned[pl.ds(pl.multiple_of(h * head_dim, head_dim), head_dim), :]
        left = jnp.concatenate([base * keep[b] for b in range(blocks)], axis=0)
        mixed[h] += jnp.dot(left, weight_s[group, h], preferred_element_type=jnp.float32)
        return carry

    lax.fori_loop(0, head_count, one_head, 0)


def fused_kernel(sides, spans, per_block, head_count, head_dim, rows, cols, *refs):
    (lists_ref, zero_ref, one_ref, two_ref, three_ref, query_ref, lw_ref, lb_ref, samples_ref,
     out_ref, blocks_v, table, ids_v, stage, fetched, index_v, index_s, point_s, corner_s, slot_s,
     spread_s, weight_s, turned, mixed, id_send, id_recv, up_send, up_recv, down_send, down_recv,
     row_send, row_recv, index_sem) = refs
    levels = (zero_ref, one_ref, two_ref)
    local_tiles = lists_ref.shape[0]
    capacity = 2
    r = lax.axis_index("row")
    c = lax.axis_index("col")
    lanes_wide = zero_ref.shape[1]
    barrier = pltpu.get_barrier_semaphore()
    for dr in range(1, rows):
        pl.semaphore_signal(barrier, inc=1, device_id={"row": lax.rem(r + dr, rows)}, device_id_type=MESH)

    @pl.when(c > 0)
    def _():
        pl.semaphore_signal(barrier, inc=1, device_id={"col": c - 1}, device_id_type=MESH)

    @pl.when(c < cols - 1)
    def _():
        pl.semaphore_signal(barrier, inc=1, device_id={"col": c + 1}, device_id_type=MESH)

    off = 0
    for level_num in range(3):
        size = local_tiles * spans[level_num]
        blocks_v[c, off:off + size, :] = levels[level_num][...]
        off += size
    span = spans[3]
    side = sides[3]
    for tile in range(local_tiles):
        rows_here = jnp.concatenate(
            [three_ref[tile * side + i].astype(jnp.float32) for i in range(side)]
            + [jnp.zeros((span - side * side, lanes_wide), jnp.float32)], axis=0
        )
        blocks_v[c, off + tile * span:off + (tile + 1) * span, :] = rows_here.astype(jnp.bfloat16)
    plan_tables(rows, cols, per_block, lists_ref, table, index_v)

    pl.semaphore_wait(barrier, rows - 1 + jnp.minimum(c, 1) + jnp.minimum(cols - 1 - c, 1))

    block_rows = blocks_v.shape[1]
    cuts = [0, 2 * spans[0], 4 * spans[0], block_rows]

    def up(block, part):
        at = blocks_v.at[block, pl.ds(cuts[part], cuts[part + 1] - cuts[part])]
        return pltpu.make_async_remote_copy(
            at, at, up_send.at[c - block, part], up_recv.at[c - block, part],
            device_id={"col": c + 1}, device_id_type=MESH,
        )

    def down(block, part):
        at = blocks_v.at[block, pl.ds(cuts[part], cuts[part + 1] - cuts[part])]
        return pltpu.make_async_remote_copy(
            at, at, down_send.at[block - c, part], down_recv.at[block - c, part],
            device_id={"col": c - 1}, device_id_type=MESH,
        )

    def came_up(block, part):
        at = blocks_v.at[block, pl.ds(cuts[part], cuts[part + 1] - cuts[part])]
        return pltpu.make_async_remote_copy(
            at, at, up_send.at[c - 1 - block, part], up_recv.at[c - 1 - block, part],
            device_id={"col": c - 1}, device_id_type=MESH,
        )

    def came_down(block, part):
        at = blocks_v.at[block, pl.ds(cuts[part], cuts[part + 1] - cuts[part])]
        return pltpu.make_async_remote_copy(
            at, at, down_send.at[block - c - 1, part], down_recv.at[block - c - 1, part],
            device_id={"col": c + 1}, device_id_type=MESH,
        )

    parts = len(cuts) - 1
    for part in range(parts):
        @pl.when(c < cols - 1)
        def _(part=part):
            up(c, part).start()

        @pl.when(c > 0)
        def _(part=part):
            down(c, part).start()

    def id_copy(dr):
        to = lax.rem(r + dr, rows)
        return pltpu.make_async_remote_copy(
            table.at[to], ids_v.at[dr], id_send.at[dr], id_recv.at[dr],
            device_id={"row": to}, device_id_type=MESH,
        )

    for dr in range(1, rows):
        id_copy(dr).start()
    ids_v[0] = table[r]
    bias = jnp.broadcast_to(lb_ref[...], (8, lb_ref.shape[1])).T[:, 0:1]

    def points_one(b, carry):
        points(head_count, b, query_ref, lw_ref, bias, samples_ref, point_s, corner_s, slot_s)
        return carry

    lax.fori_loop(0, local_tiles, points_one, 0)
    index_copy = pltpu.make_async_copy(index_v, index_s, index_sem)
    index_copy.start()
    for dr in range(1, rows):
        id_copy(dr).wait()

    def arrive(block):
        for part in range(parts):
            @pl.when(block < c)
            def _(part=part):
                came_up(block, part).wait_recv()

                @pl.when(c < cols - 1)
                def _():
                    up(block, part).start()

            @pl.when(block > c)
            def _(part=part):
                came_down(block, part).wait_recv()

                @pl.when(c > 0)
                def _():
                    down(block, part).start()

    def row_copy(block, dr, level_num):
        span = spans[level_num]
        first = capacity * sum(spans[:level_num])
        off = rows * first
        size = capacity * span
        return pltpu.make_async_remote_copy(
            stage.at[block, dr - 1, pl.ds(first, size)],
            fetched.at[block, pl.ds(pl.multiple_of(off + r * size, size), size)],
            row_send.at[block, dr, level_num], row_recv.at[block, dr, level_num],
            device_id={"row": lax.rem(r - dr + rows, rows)}, device_id_type=MESH,
        )

    def pick(block):
        for turn in range(rows):
            dr = (turn + 1) % rows
            off = 0
            for level_num in range(LEVELS):
                span = spans[level_num]
                size = capacity * span
                for place in range(capacity):
                    asked = jnp.broadcast_to(
                        ids_v[dr, level_num, pl.ds(block * capacity + place, 1), :], (PACK, lanes_wide)
                    )
                    total = None
                    for tile in range(local_tiles):
                        mask = jnp.where(asked == tile, 1.0, 0.0).astype(jnp.bfloat16)
                        first = local_tiles * off + tile * span
                        part = blocks_v[block, first:first + span, :].reshape(
                            span // PACK, PACK, lanes_wide) * mask[None]
                        total = part if total is None else total + part
                    total = total.reshape(span, lanes_wide)
                    if dr == 0:
                        at = pl.multiple_of(rows * capacity * off + r * size + place * span, span)
                        fetched[block, pl.ds(at, span), :] = total
                    else:
                        at = capacity * off + place * span
                        stage[block, dr - 1, at:at + span, :] = total
                if dr != 0:
                    row_copy(block, dr, level_num).start()
                off += span

    def settle(block):
        for dr in range(1, rows):
            for level_num in range(LEVELS):
                row_copy(block, dr, level_num).wait_recv()

    def spread_one(step, carry):
        spread(sides, spans, head_count, step, point_s, corner_s, spread_s)
        return carry

    def weigh(block):
        weigh_slots(spans, per_block, head_count, rows, cols, block, index_s, slot_s, spread_s, weight_s)

    def mix(block):
        settle(block)
        mix_slots(spans, per_block, head_count, head_dim, rows, cols, local_tiles, block, index_s,
                  fetched, turned, weight_s, mixed)

    order = group_order(c, cols)
    mixed[...] = jnp.zeros_like(mixed)
    pick(order[0])
    lax.fori_loop(0, local_tiles * head_count, spread_one, 0)
    index_copy.wait()
    for g in range(1, cols):
        arrive(order[g])
        pick(order[g])
        weigh(order[g - 1])
        if g > 1:
            mix(order[g - 2])
    weigh(order[cols - 1])
    mix(order[cols - 2])
    mix(order[cols - 1])

    for b in range(local_tiles):
        whole = mixed[:, b * head_dim:(b + 1) * head_dim, :].reshape(head_count * head_dim, mixed.shape[2])
        size = mixed.shape[2]
        out_ref[b * size:(b + 1) * size, :] = whole.T.astype(jnp.bfloat16)

    for dr in range(1, rows):
        for block in range(cols):
            for level_num in range(LEVELS):
                row_copy(block, dr, level_num).wait_send()
    for block in range(cols):
        for part in range(parts):
            @pl.when((block <= c) & (c < cols - 1))
            def _(block=block, part=part):
                up(block, part).wait_send()

            @pl.when((block >= c) & (c > 0))
            def _(block=block, part=part):
                down(block, part).wait_send()


def fused_attention(queries, level_blocks, tile_lists, samples, logit_weight, logit_bias, sides, spans):
    rows = lax.axis_size("row")
    cols = lax.axis_size("col")
    tile_rows, tile_cols, level_count, per_block = tile_lists.shape
    local_tiles = tile_rows * tile_cols
    requests = local_tiles * per_block
    channels = level_blocks[0].shape[2]
    lanes = samples.shape[2]
    head_count = lanes // (LEVELS * POINTS)
    head_dim = channels // head_count
    pixels = spans[0]
    tile_span = sum(spans)
    capacity = requests // (rows * cols)
    depth = rows * capacity * tile_span
    flat = [level.reshape(-1, channels) for level in level_blocks[:3]]
    vmem = pl.BlockSpec(memory_space=pltpu.VMEM)
    dma = pltpu.SemaphoreType.DMA
    parts = 3
    return pl.pallas_call(
        functools.partial(fused_kernel, sides, spans, per_block, head_count, head_dim, rows, cols),
        out_shape=jax.ShapeDtypeStruct((local_tiles * pixels, channels), jnp.bfloat16),
        in_specs=[vmem] * 9,
        out_specs=vmem,
        scratch_shapes=[
            pltpu.VMEM((cols, local_tiles * tile_span, channels), jnp.bfloat16),
            pltpu.VMEM((rows, LEVELS, requests // rows, channels), jnp.int32),
            pltpu.VMEM((rows, LEVELS, requests // rows, channels), jnp.int32),
            pltpu.VMEM((cols, rows - 1, capacity * tile_span, channels), jnp.bfloat16),
            pltpu.VMEM((cols, depth, channels), jnp.bfloat16),
            pltpu.VMEM((8, 128), jnp.int32),
            pltpu.SMEM((8, 128), jnp.int32),
            pltpu.VMEM((local_tiles, 2, lanes, pixels), jnp.int32),
            pltpu.VMEM((local_tiles, 4, lanes, pixels), jnp.float32),
            pltpu.VMEM((local_tiles, lanes, pixels), jnp.float32),
            pltpu.VMEM((local_tiles * head_count, POINTS, tile_span, pixels), jnp.bfloat16),
            pltpu.VMEM((cols, head_count, depth, pixels), jnp.bfloat16),
            pltpu.VMEM((channels, depth), jnp.bfloat16),
            pltpu.VMEM((head_count, local_tiles * head_dim, pixels), jnp.float32),
            dma((rows,)), dma((rows,)),
            dma((cols, parts)), dma((cols, parts)), dma((cols, parts)), dma((cols, parts)),
            dma((cols, rows, LEVELS)), dma((cols, rows, LEVELS)),
            dma,
        ],
        compiler_params=pltpu.CompilerParams(
            collective_id=1, has_side_effects=True, vmem_limit_bytes=60 * 1024 * 1024
        ),
        name="fused",
    )(
        tile_lists.reshape(local_tiles, level_count, per_block), *flat, level_blocks[3],
        queries.reshape(local_tiles, pixels, queries.shape[2]), logit_weight.T, logit_bias[None, :],
        samples.reshape(local_tiles, pixels, lanes),
    )


def on_device(
    queries,
    level_zero,
    level_one,
    level_two,
    level_three,
    tile_lists,
    samples,
    logit_weight,
    logit_bias,
    output_weight,
    output_bias,
    norm_gain,
    norm_shift,
):
    level_blocks = (level_zero, level_one, level_two, level_three)
    tile_rows, tile_cols, level_count, per_block = tile_lists.shape
    local_tiles = tile_rows * tile_cols
    requests = local_tiles * per_block
    channels = level_zero.shape[2]
    width_all = queries.shape[2]
    tile_side = level_zero.shape[0] // tile_rows
    pixels = tile_side * tile_side
    sides = [level.shape[0] // tile_rows for level in level_blocks]
    spans = [max(PACK, side * side) for side in sides]
    peer_count = lax.axis_size("row") * lax.axis_size("col")
    full = requests == 2 * peer_count and tile_cols == 1 and sides == [16, 8, 4, 2]
    full = full and all(power_of_two(n) for n in (tile_rows, lax.axis_size("col"), per_block))
    attention = fused_attention if full else gathered_attention
    attn_out = attention(
        queries, level_blocks, tile_lists, samples, logit_weight, logit_bias, sides, spans
    )
    queries_blocked = to_blocks(queries, tile_rows, tile_cols, tile_side)

    head_index = lax.axis_index("head")
    full_attn = lax.all_gather(attn_out, "head", axis=1, tiled=True)
    pre_norm = (
        queries_blocked.reshape(local_tiles * pixels, width_all).astype(jnp.float32)
        + jnp.dot(full_attn, output_weight, preferred_element_type=jnp.float32)
        + output_bias
    )
    row_mean = jnp.mean(pre_norm, axis=1, keepdims=True)
    centered = pre_norm - row_mean
    variance = jnp.mean(centered * centered, axis=1, keepdims=True)
    own_part = lax.dynamic_slice_in_dim(centered, head_index * channels, channels, 1)
    normalized = own_part * lax.rsqrt(variance + 1e-05)
    updated = (normalized * norm_gain + norm_shift).astype(jnp.bfloat16)
    updated = updated.reshape(tile_rows, tile_cols, tile_side, tile_side, channels).transpose(
        0, 2, 1, 3, 4
    )
    return updated.reshape(tile_rows * tile_side, tile_cols * tile_side, channels)


def solution(mesh):
    in_specs = (
        P("row", "col", None),
        P("row", "col", "head"),
        P("row", "col", "head"),
        P("row", "col", "head"),
        P("row", "col", "head"),
        P("row", "col", None, None),
        P("row", "col", "head"),
        P(None, "head"),
        P("head"),
        P(),
        P(),
        P("head"),
        P("head"),
    )
    out_specs = P("row", "col", "head")
    return jax.shard_map(
        on_device, mesh=mesh, in_specs=in_specs, out_specs=out_specs, check_vma=False
    )
```

```python
import functools

import jax
import jax.numpy as jnp
from jax import lax
from jax.experimental import pallas as pl
from jax.experimental.pallas import tpu as pltpu
from jax.sharding import PartitionSpec as P

LEVELS = 4
POINTS = 4
PACK = 16
MESH = pl.DeviceIdType.MESH


def to_blocks(source, tile_rows, tile_cols, tile_side):
    channels = source.shape[2]
    shaped = source.reshape(tile_rows, tile_side, tile_cols, tile_side, channels)
    return shaped.transpose(0, 2, 1, 3, 4).reshape(
        tile_rows * tile_cols, tile_side * tile_side, channels
    )


def hat(index, start, low, high):
    return jnp.where(index == start, low, jnp.where(index == start + 1, high, 0.0))


def prepare(head_count, b, query_ref, lw_ref, lb_ref, samples_ref, point_s, corner_s):
    queries_here = query_ref.shape[1]
    hits = LEVELS * POINTS
    logits = lax.dot_general(
        lw_ref[...], query_ref[b], (((1,), (1,)), ((), ())), preferred_element_type=jnp.float32
    ) + lb_ref[...]
    logits = logits.reshape(head_count, hits, queries_here)
    shifted = jnp.exp(logits - jnp.max(logits, axis=1, keepdims=True))
    attend = shifted / jnp.sum(shifted, axis=1, keepdims=True)
    attend = attend.reshape(head_count * hits, queries_here)
    packed = samples_ref[b].T
    pos_row = (packed >> 12) & 4095
    pos_col = packed & 4095
    frac_row = (pos_row & 255).astype(jnp.float32) * (1.0 / 256.0)
    frac_col = (pos_col & 255).astype(jnp.float32) * (1.0 / 256.0)
    point_s[b, 0] = packed >> 24
    point_s[b, 1] = pos_row >> 8
    point_s[b, 2] = pos_col >> 8
    corner_s[b, 0] = attend * (1.0 - frac_row)
    corner_s[b, 1] = attend * frac_row
    corner_s[b, 2] = 1.0 - frac_col
    corner_s[b, 3] = frac_col


def weigh(sides, spans, per_block, b, h, slab, point_s, corner_s, mask_s, weight_s):
    hits = LEVELS * POINTS
    queries_here = weight_s.shape[2]
    lane_row = lax.broadcasted_iota(jnp.int32, (PACK, queries_here), 0)
    slot_row = lax.broadcasted_iota(jnp.int32, (per_block, queries_here), 0)
    level_off = 0
    for level_num in range(LEVELS):
        side = sides[level_num]
        span = spans[level_num]
        rows = [pl.ds(h * hits + level_num * POINTS + p, 1) for p in range(POINTS)]
        for p in range(POINTS):
            mask_s[p * per_block:(p + 1) * per_block, :] = jnp.where(
                slot_row == point_s[b, 0, rows[p], :], 1.0, 0.0
            )
        cols = [
            hat(lane_row % side, point_s[b, 2, rows[p], :], corner_s[b, 2, rows[p], :],
                corner_s[b, 3, rows[p], :])
            for p in range(POINTS)
        ]
        rows_per_chunk = PACK // side

        def chunk(step, carry, rows=rows, cols=cols, side=side, span=span,
                  level_off=level_off, rows_per_chunk=rows_per_chunk):
            parts = []
            for p in range(POINTS):
                index = step * rows_per_chunk
                start = point_s[b, 1, rows[p], :]
                low = corner_s[b, 0, rows[p], :]
                high = corner_s[b, 1, rows[p], :]
                if rows_per_chunk > 1:
                    across = hat(index + lane_row // side, start, low, high)
                else:
                    across = jnp.where(
                        start == index, low, jnp.where(start == index - 1, high, 0.0)
                    )
                parts.append(cols[p] * across)
            for k in range(per_block):
                total = parts[0] * mask_s[k:k + 1, :]
                for p in range(1, POINTS):
                    total = total + parts[p] * mask_s[p * per_block + k:p * per_block + k + 1, :]
                where = pl.multiple_of(level_off + k * span + step * PACK, PACK)
                weight_s[slab, pl.ds(where, PACK), :] = total.astype(jnp.bfloat16)
            return carry

        chunks = span // PACK
        if chunks == 1:
            chunk(0, 0)
        else:
            lax.fori_loop(0, chunks, chunk, 0)
        level_off += span * per_block


def exchange_kernel(sides, spans, per_block, head_count, rows, cols, capacity, local_tiles, *refs):
    (table_ref, tiles_ref, query_ref, lw_ref, lb_ref, samples_ref, fetched_ref, weights_ref) = refs[:8]
    refs = refs[8:]
    held = refs[:cols - 1]
    (ids_v, stage, point_s, corner_s, mask_s, weight_s, id_send, id_recv, col_send, col_recv,
     row_send, row_recv, own_sem, ids_sem, weight_sem) = refs[cols - 1:]
    r = lax.axis_index("row")
    c = lax.axis_index("col")
    lanes_wide = tiles_ref.shape[1]
    barrier = pltpu.get_barrier_semaphore()
    for dc in range(1, cols):
        pl.semaphore_signal(barrier, inc=1, device_id={"col": lax.rem(c + dc, cols)}, device_id_type=MESH)
    for dr in range(1, rows):
        pl.semaphore_signal(barrier, inc=1, device_id={"row": lax.rem(r + dr, rows)}, device_id_type=MESH)
    pl.semaphore_wait(barrier, cols + rows - 2)

    id_copies = []
    for dr in range(1, rows):
        to = lax.rem(r + dr, rows)
        copy = pltpu.make_async_remote_copy(
            table_ref.at[to], ids_v.at[dr], id_send.at[dr], id_recv.at[dr],
            device_id={"row": to}, device_id_type=MESH,
        )
        copy.start()
        id_copies.append(copy)
    col_copies = []
    for dc in range(1, cols):
        copy = pltpu.make_async_remote_copy(
            tiles_ref, held[dc - 1], col_send.at[dc], col_recv.at[dc],
            device_id={"col": lax.rem(c + dc, cols)}, device_id_type=MESH,
        )
        copy.start()
        col_copies.append(copy)
    own_ids = pltpu.make_async_copy(table_ref.at[r], ids_v.at[0], ids_sem)
    own_ids.start()
    own_ids.wait()
    for copy in id_copies:
        copy.wait()

    def pick(dc):
        owner_col = lax.rem(c - dc + cols, cols)
        source = tiles_ref if dc == 0 else held[dc - 1]
        out_at = (r * cols + owner_col) * capacity
        copies = []
        for turn in range(rows):
            dr = (turn + 1) % rows
            for place in range(capacity):
                off = 0
                for level_num in range(LEVELS):
                    span = spans[level_num]
                    at = (owner_col * capacity + place) * LEVELS + level_num
                    asked = jnp.broadcast_to(ids_v[dr, pl.ds(at, 1), :], (PACK, lanes_wide))
                    shape = (span // PACK, PACK, lanes_wide)
                    total = None
                    for tile in range(local_tiles):
                        mask = jnp.where(asked == tile, 1.0, 0.0).astype(jnp.bfloat16)
                        first = local_tiles * off + tile * span
                        part = source[first:first + span, :].reshape(shape) * mask[None]
                        total = part if total is None else total + part
                    stage[dr, dc, place, off:off + span, :] = total.reshape(span, lanes_wide)
                    off += span
            target = fetched_ref.at[pl.ds(out_at, capacity)]
            if dr == 0:
                copy = pltpu.make_async_copy(stage.at[dr, dc], target, own_sem.at[dc])
            else:
                copy = pltpu.make_async_remote_copy(
                    stage.at[dr, dc], target, row_send.at[dr, dc], row_recv.at[dr, dc],
                    device_id={"row": lax.rem(r - dr + rows, rows)}, device_id_type=MESH,
                )
            copy.start()
            copies.append(copy)
        return copies

    copies = pick(0)

    def prepare_one(b, carry):
        prepare(head_count, b, query_ref, lw_ref, lb_ref, samples_ref, point_s, corner_s)
        return carry

    lax.fori_loop(0, local_tiles, prepare_one, 0)

    def store(step, slab):
        return pltpu.make_async_copy(
            weight_s.at[slab], weights_ref.at[step // head_count, step % head_count],
            weight_sem.at[slab],
        )

    def weigh_one(step, carry):
        slab = step % 2

        @pl.when(step >= 2)
        def _():
            store(step - 2, slab).wait()

        weigh(sides, spans, per_block, step // head_count, step % head_count, slab,
              point_s, corner_s, mask_s, weight_s)
        store(step, slab).start()
        return carry

    steps = local_tiles * head_count
    done = 0
    for dc in range(1, cols):
        until = steps * dc // (cols - 1)
        if until > done:
            lax.fori_loop(done, until, weigh_one, 0)
        done = until
        col_copies[dc - 1].wait()
        copies += pick(dc)
    for step in range(max(0, steps - 2), steps):
        store(step, step % 2).wait()
    for copy in copies:
        copy.wait()


def mix_kernel(spans, per_block, head_count, head_dim, pos_ref, fetched_ref, upper_ref, lower_ref,
               out_ref,
               values, values_t, mixed, sem):
    block = pl.program_id(0)
    h = pl.program_id(1)
    blocks = pl.num_programs(0)

    def fetch(which):
        off = 0
        src = 0
        for level_num in range(LEVELS):
            span = spans[level_num]
            for k in range(per_block):
                pltpu.make_async_copy(
                    fetched_ref.at[pos_ref[level_num, which * per_block + k], pl.ds(src, span), :],
                    values.at[which % 2, pl.ds(off, span), :],
                    sem.at[which % 2],
                ).start()
                off += span
            src += span

    @pl.when((h == 0) & (block == 0))
    def _():
        fetch(block)

    @pl.when(h == 0)
    def _():
        side = block % 2
        pltpu.make_async_copy(values.at[side], values.at[side], sem.at[side]).wait()
        values_t[...] = values[side].T.reshape(values_t.shape)

        @pl.when(block + 1 < blocks)
        def _():
            fetch(block + 1)

    half = upper_ref.shape[2]
    mixed[h] = jnp.dot(
        values_t[h, :, :half], upper_ref[0, 0], preferred_element_type=jnp.float32
    ) + jnp.dot(values_t[h, :, half:], lower_ref[0, 0], preferred_element_type=jnp.float32)

    @pl.when(h == head_count - 1)
    def _():
        whole = mixed[...].reshape(head_count * head_dim, mixed.shape[2])
        out_ref[...] = whole.T.astype(jnp.bfloat16)


def gathered_attention(queries, level_blocks, tile_lists, samples, logit_weight, logit_bias, sides, spans):
    row_count = lax.axis_size("row")
    col_count = lax.axis_size("col")
    peer_count = row_count * col_count
    tile_rows, tile_cols, level_count, per_block = tile_lists.shape
    local_tiles = tile_rows * tile_cols
    requests = local_tiles * per_block
    capacity = max(2, (requests + peer_count - 1) // peer_count)
    slots = peer_count * capacity
    grid_cols = tile_cols * col_count
    channels = level_blocks[0].shape[2]
    head_count = samples.shape[2] // (LEVELS * POINTS)
    head_dim = channels // head_count
    tile_side = sides[0]
    pixels = tile_side * tile_side
    tile_span = sum(spans)
    depth = per_block * tile_span

    wanted = tile_lists.transpose(2, 0, 1, 3).reshape(level_count, requests)
    grid_row = wanted // grid_cols
    grid_col = wanted % grid_cols
    owner_dev = grid_row // tile_rows * col_count + grid_col // tile_cols
    local_index = grid_row % tile_rows * tile_cols + grid_col % tile_cols
    order = jnp.arange(requests, dtype=jnp.int32)
    earlier = (owner_dev[:, :, None] == owner_dev[:, None, :]) & (order[None, :] < order[:, None])
    positions = owner_dev * capacity + jnp.sum(earlier.astype(jnp.int32), axis=2)
    slot_order = jnp.arange(slots, dtype=jnp.int32)
    named = positions[:, None, :] == slot_order[None, :, None]
    slot_table = jnp.max(jnp.where(named, local_index[:, None, :], -1), axis=2)
    table = jnp.maximum(slot_table, 0).reshape(level_count, row_count, col_count * capacity)
    table = table.transpose(1, 2, 0).reshape(row_count, col_count * capacity * level_count, 1)
    table_rows = table.shape[1]
    table = jnp.broadcast_to(table, (row_count, table_rows, channels))

    tiles_local = []
    for level_num in range(level_count):
        tiles = to_blocks(level_blocks[level_num], tile_rows, tile_cols, sides[level_num])
        short = spans[level_num] - tiles.shape[1]
        if short > 0:
            tiles = jnp.pad(tiles, ((0, 0), (0, short), (0, 0)))
        tiles_local.append(tiles.reshape(local_tiles * spans[level_num], channels))
    tiles_local = jnp.concatenate(tiles_local, axis=0)

    queries_blocked = to_blocks(queries, tile_rows, tile_cols, tile_side)
    samples_blocked = to_blocks(samples, tile_rows, tile_cols, tile_side)
    lanes = head_count * LEVELS * POINTS
    vmem = pl.BlockSpec(memory_space=pltpu.VMEM)
    whole = pl.BlockSpec(memory_space=pl.ANY)
    dma = pltpu.SemaphoreType.DMA
    fetched, weights = pl.pallas_call(
        functools.partial(exchange_kernel, sides, spans, per_block, head_count, row_count,
                          col_count, capacity, local_tiles),
        out_shape=(
            jax.ShapeDtypeStruct((slots, tile_span, channels), jnp.bfloat16),
            jax.ShapeDtypeStruct((local_tiles, head_count, depth, pixels), jnp.bfloat16),
        ),
        in_specs=[vmem] * 6,
        out_specs=(whole, whole),
        scratch_shapes=[
            pltpu.VMEM((local_tiles * tile_span, channels), jnp.bfloat16)
            for _ in range(col_count - 1)
        ] + [
            pltpu.VMEM((row_count, table_rows, channels), jnp.int32),
            pltpu.VMEM((row_count, col_count, capacity, tile_span, channels), jnp.bfloat16),
            pltpu.VMEM((local_tiles, 3, lanes, pixels), jnp.int32),
            pltpu.VMEM((local_tiles, 4, lanes, pixels), jnp.float32),
            pltpu.VMEM((POINTS * per_block, pixels), jnp.float32),
            pltpu.VMEM((2, depth, pixels), jnp.bfloat16),
            dma((row_count,)), dma((row_count,)), dma((col_count,)), dma((col_count,)),
            dma((row_count, col_count)), dma((row_count, col_count)), dma((col_count,)),
            dma, dma((2,)),
        ],
        compiler_params=pltpu.CompilerParams(
            collective_id=0, has_side_effects=True, vmem_limit_bytes=60 * 1024 * 1024
        ),
        cost_estimate=pl.CostEstimate(
            flops=8 * local_tiles * head_count * depth * pixels * POINTS,
            bytes_accessed=2 * local_tiles * head_count * depth * pixels, transcendentals=0,
        ),
        name="exchange",
    )(table, tiles_local, queries_blocked, logit_weight.T, logit_bias[:, None], samples_blocked)

    attn_out = pl.pallas_call(
        functools.partial(mix_kernel, spans, per_block, head_count, head_dim),
        grid_spec=pltpu.PrefetchScalarGridSpec(
            num_scalar_prefetch=1,
            grid=(local_tiles, head_count),
            in_specs=[
                pl.BlockSpec(memory_space=pl.ANY),
                pl.BlockSpec((1, 1, depth // 2, pixels), lambda b, h, pos: (b, h, 0, 0)),
                pl.BlockSpec((1, 1, depth // 2, pixels), lambda b, h, pos: (b, h, 1, 0)),
            ],
            out_specs=pl.BlockSpec((pixels, channels), lambda b, h, pos: (b, 0)),
            scratch_shapes=[
                pltpu.VMEM((2, depth, channels), jnp.bfloat16),
                pltpu.VMEM((head_count, head_dim, depth), jnp.bfloat16),
                pltpu.VMEM((head_count, head_dim, pixels), jnp.float32),
                pltpu.SemaphoreType.DMA((2,)),
            ],
        ),
        out_shape=jax.ShapeDtypeStruct((local_tiles * pixels, channels), jnp.bfloat16),
        compiler_params=pltpu.CompilerParams(
            dimension_semantics=("arbitrary", "arbitrary"), vmem_limit_bytes=60 * 1024 * 1024
        ),
        cost_estimate=pl.CostEstimate(
            flops=2 * local_tiles * depth * pixels * channels,
            bytes_accessed=2 * local_tiles * head_count * depth * pixels, transcendentals=0,
        ),
        name="mix",
    )(positions, fetched, weights, weights)
    return attn_out


def power_of_two(n):
    return n > 0 and n & (n - 1) == 0


def group_order(c, cols):
    near = jnp.minimum(c, cols - 1 - c)
    order = [c]
    for g in range(1, cols):
        both = c - (g + 1) // 2 if g % 2 else c + g // 2
        one = jnp.where(c < cols - 1 - c, c + g - near, c - g + near)
        order.append(jnp.where(g <= 2 * near, both, one))
    return order


def plan_tables(rows, cols, per_block, lists_ref, table, index_v):
    blocks = lists_ref.shape[0]
    wanted = jnp.concatenate([lists_ref[b] for b in range(blocks)], axis=1)
    requests = wanted.shape[1]
    tile_rows = blocks
    col_bits = cols.bit_length() - 1
    row_bits = tile_rows.bit_length() - 1
    shape = (requests, requests)
    down = lax.broadcasted_iota(jnp.int32, shape, 0)
    along = lax.broadcasted_iota(jnp.int32, shape, 1)
    capacity = requests // (rows * cols)
    for level_num in range(LEVELS):
        here = jnp.broadcast_to(wanted[level_num:level_num + 1, :], shape)
        own_here = ((here >> (col_bits + row_bits)) << col_bits) + (here & (cols - 1))
        local_here = (here >> col_bits) & (tile_rows - 1)
        same = own_here == own_here.T
        place_here = jnp.sum(jnp.where(same & (down < along), 1, 0), axis=0, keepdims=True)
        slot_here = own_here * capacity + place_here
        asked = jnp.sum(
            jnp.where(slot_here == down, local_here.astype(jnp.float32), 0.0), axis=1, keepdims=True
        )
        asked = jnp.broadcast_to(asked, (requests, table.shape[3])).astype(jnp.int32)
        table[:, level_num] = asked.reshape(rows, requests // rows, table.shape[3])
        filled = jnp.sum(jnp.where(slot_here.T == along, down, 0), axis=0, keepdims=True)
        index_v[level_num:level_num + 1, 0:requests] = filled


def points(head_count, b, query_ref, lw_ref, bias, samples_ref, point_s, corner_s, slot_s):
    queries_here = query_ref.shape[1]
    hits = LEVELS * POINTS
    logits = lax.dot_general(
        lw_ref[...], query_ref[b], (((1,), (1,)), ((), ())), preferred_element_type=jnp.float32
    ) + bias
    logits = logits.reshape(head_count, hits, queries_here)
    shifted = jnp.exp(logits - jnp.max(logits, axis=1, keepdims=True))
    attend = shifted / jnp.sum(shifted, axis=1, keepdims=True)
    attend = attend.reshape(head_count * hits, queries_here)
    packed = samples_ref[b].T
    pos_row = (packed >> 12) & 4095
    pos_col = packed & 4095
    frac_row = (pos_row & 255).astype(jnp.float32) * (1.0 / 256.0)
    frac_col = (pos_col & 255).astype(jnp.float32) * (1.0 / 256.0)
    point_s[b, 0] = pos_row >> 8
    point_s[b, 1] = pos_col >> 8
    corner_s[b, 0] = attend * (1.0 - frac_row)
    corner_s[b, 1] = attend * frac_row
    corner_s[b, 2] = 1.0 - frac_col
    corner_s[b, 3] = frac_col
    slot_s[b] = (packed >> 24).astype(jnp.float32)


def hats(start, low, high, count):
    here = [start == i for i in range(count)]
    out = [jnp.where(here[0], low, 0.0)]
    for i in range(1, count):
        out.append(jnp.where(here[i], low, jnp.where(here[i - 1], high, 0.0)))
    return out


def weigh_block(sides, spans, per_block, head_count, step, point_s, corner_s, slot_s, down_s, spread_s,
                weight_s):
    hits = LEVELS * POINTS
    queries_here = spread_s.shape[2]
    b = step // head_count
    h = step % head_count
    half = PACK // 2
    lane_row = lax.broadcasted_iota(jnp.int32, (PACK, queries_here), 0)
    off = 0
    for level_num in range(LEVELS):
        side = sides[level_num]
        span = spans[level_num]
        for p in range(POINTS):
            row = pl.ds(h * hits + level_num * POINTS + p, 1)
            across = hat(lane_row % side, point_s[b, 1, row, :], corner_s[b, 2, row, :],
                         corner_s[b, 3, row, :])
            down = hat(lane_row // side if side < half else lane_row, point_s[b, 0, row, :],
                       corner_s[b, 0, row, :], corner_s[b, 1, row, :])
            if side >= half:
                at_down = (level_num * POINTS + p) * PACK
                down_s[at_down:at_down + PACK, :] = down
                for chunk in range(span // PACK):
                    parts = []
                    for part in range(2):
                        at = chunk * PACK + part * half
                        col = at % side if side > half else part * half
                        line = at_down + at // side
                        parts.append(across[col:col + half, :] * down_s[line:line + 1, :])
                    total = jnp.concatenate(parts, axis=0).astype(jnp.bfloat16)
                    spread_s[p, off + chunk * PACK:off + (chunk + 1) * PACK, :] = total
            else:
                spread_s[p, off:off + PACK, :] = (across * down).astype(jnp.bfloat16)
        off += span
    off = 0
    quad = 4
    one = jnp.ones((PACK, queries_here), jnp.bfloat16)
    none = jnp.zeros((PACK, queries_here), jnp.bfloat16)
    for level_num in range(LEVELS):
        span = spans[level_num]
        slots = []
        for p in range(POINTS):
            mine = slot_s[b, pl.ds(h * hits + level_num * POINTS + p, 1), :]
            slots.append(jnp.broadcast_to(mine, (PACK, queries_here)).astype(jnp.bfloat16))
        for first in range(0, per_block, quad):
            masks = []
            for k in range(first, first + quad):
                label = jnp.full((PACK, queries_here), k, jnp.bfloat16)
                masks.append([jnp.where(slots[p] == label, one, none) for p in range(POINTS)])
            for chunk in range(span // PACK):
                pieces = [spread_s[p, off + chunk * PACK:off + (chunk + 1) * PACK, :] for p in range(POINTS)]
                for k in range(first, first + quad):
                    total = pieces[0] * masks[k - first][0]
                    for p in range(1, POINTS):
                        total = total + pieces[p] * masks[k - first][p]
                    weight_s[level_num][step * per_block + k, chunk * PACK:(chunk + 1) * PACK, :] = total
        off += span


def mix_slots(spans, per_block, head_count, head_dim, rows, cols, blocks, group, index_s, fetched,
              turned, keep_s, weight_s, mixed, finish):
    capacity = 2
    units = rows * capacity
    lanes = 128
    block_bits = per_block.bit_length() - 1
    requests = blocks * per_block
    turned[...] = fetched[group].T
    lane = lax.broadcasted_iota(jnp.int32, (1, lanes), 1)

    def entry_of(level_num, unit):
        slot = (unit // capacity * cols + group) * capacity + unit % capacity
        return index_s[level_num, slot] & (requests - 1)

    owners = []
    for level_num in range(LEVELS):
        span = spans[level_num]
        block_of = [entry_of(level_num, unit) >> block_bits for unit in range(units)]
        for start in range(0, units * span, lanes):
            first = start // span
            last = (start + lanes - 1) // span
            value = jnp.full((1, lanes), block_of[first], jnp.int32)
            for unit in range(first + 1, last + 1):
                value = jnp.where(lane >= unit * span - start, block_of[unit], value)
            owners.append(value)
    owner_row = jnp.concatenate(owners, axis=1)
    for b in range(blocks):
        keep_s[b] = jnp.broadcast_to(
            jnp.where(owner_row == b, 1.0, 0.0), (PACK, owner_row.shape[1])
        ).astype(jnp.bfloat16)

    def one_head(h, carry):
        left = jnp.concatenate([
            turned[pl.ds(pl.multiple_of(h * head_dim + half, PACK), PACK), :] * keep_s[b]
            for b in range(blocks) for half in range(0, head_dim, PACK)
        ], axis=0)
        right = []
        for level_num in range(LEVELS):
            for unit in range(units):
                entry = entry_of(level_num, unit)
                source = (entry >> block_bits) * head_count + h
                right.append(weight_s[level_num][source * per_block + (entry & (per_block - 1))])
        right = jnp.concatenate(right, axis=0)
        total = mixed[h] + jnp.dot(left, right, preferred_element_type=jnp.float32)
        finish(h, total)
        return carry

    lax.fori_loop(0, head_count, one_head, 0)


def fused_kernel(sides, spans, per_block, head_count, head_dim, rows, cols, *refs):
    sources, refs = refs[:11], refs[11:]
    out_ref, refs = refs[0], refs[1:]
    held, refs = refs[:8], refs[8:]
    (lists_ref, three_ref, query_ref, lw_ref, lb_ref, samples_ref, ow_ref, ob_ref) = held
    (blocks_v, table, ids_v, stage, fetched, index_v, index_s, point_s,
     corner_s, slot_s, down_s, spread_s, weight_0, weight_1, weight_2, weight_3, turned, keep_s, mixed,
     attn_own, attn_other, id_send, id_recv, up_send, up_recv, down_send, down_recv, row_send, row_recv,
     head_send, head_recv, index_sem, in_sem) = refs
    weight_s = (weight_0, weight_1, weight_2, weight_3)
    local_tiles = lists_ref.shape[0]
    capacity = 2
    r = lax.axis_index("row")
    c = lax.axis_index("col")
    head = lax.axis_index("head")
    lanes_wide = blocks_v.shape[2]
    targets = []
    off = 0
    for level_num in range(3):
        size = local_tiles * spans[level_num]
        targets.append(blocks_v.at[c, pl.ds(off, size)])
        off += size
    loads = [
        pltpu.make_async_copy(source, target, in_sem.at[i])
        for i, (source, target) in enumerate(zip(sources, targets + list(held)))
    ]
    for load in loads:
        load.start()
    barrier = pltpu.get_barrier_semaphore()
    pl.semaphore_signal(barrier, inc=1, device_id={"head": 1 - head}, device_id_type=MESH)
    for dr in range(1, rows):
        pl.semaphore_signal(barrier, inc=1, device_id={"row": lax.rem(r + dr, rows)}, device_id_type=MESH)

    @pl.when(c > 0)
    def _():
        pl.semaphore_signal(barrier, inc=1, device_id={"col": c - 1}, device_id_type=MESH)

    @pl.when(c < cols - 1)
    def _():
        pl.semaphore_signal(barrier, inc=1, device_id={"col": c + 1}, device_id_type=MESH)

    for load in loads[3:5]:
        load.wait()
    span = spans[3]
    side = sides[3]
    for tile in range(local_tiles):
        rows_here = jnp.concatenate(
            [three_ref[tile * side + i].astype(jnp.float32) for i in range(side)]
            + [jnp.zeros((span - side * side, lanes_wide), jnp.float32)], axis=0
        )
        blocks_v[c, off + tile * span:off + (tile + 1) * span, :] = rows_here.astype(jnp.bfloat16)
    plan_tables(rows, cols, per_block, lists_ref, table, index_v)

    for load in loads[:3]:
        load.wait()
    pl.semaphore_wait(barrier, rows + jnp.minimum(c, 1) + jnp.minimum(cols - 1 - c, 1))

    block_rows = blocks_v.shape[1]
    cuts = [0, 2 * spans[0], 4 * spans[0], block_rows]

    def up(block, part):
        at = blocks_v.at[block, pl.ds(cuts[part], cuts[part + 1] - cuts[part])]
        return pltpu.make_async_remote_copy(
            at, at, up_send.at[c - block, part], up_recv.at[c - block, part],
            device_id={"col": c + 1}, device_id_type=MESH,
        )

    def down(block, part):
        at = blocks_v.at[block, pl.ds(cuts[part], cuts[part + 1] - cuts[part])]
        return pltpu.make_async_remote_copy(
            at, at, down_send.at[block - c, part], down_recv.at[block - c, part],
            device_id={"col": c - 1}, device_id_type=MESH,
        )

    def came_up(block, part):
        at = blocks_v.at[block, pl.ds(cuts[part], cuts[part + 1] - cuts[part])]
        return pltpu.make_async_remote_copy(
            at, at, up_send.at[c - 1 - block, part], up_recv.at[c - 1 - block, part],
            device_id={"col": c - 1}, device_id_type=MESH,
        )

    def came_down(block, part):
        at = blocks_v.at[block, pl.ds(cuts[part], cuts[part + 1] - cuts[part])]
        return pltpu.make_async_remote_copy(
            at, at, down_send.at[block - c - 1, part], down_recv.at[block - c - 1, part],
            device_id={"col": c + 1}, device_id_type=MESH,
        )

    parts = len(cuts) - 1
    for part in range(parts):
        @pl.when(c < cols - 1)
        def _(part=part):
            up(c, part).start()

        @pl.when(c > 0)
        def _(part=part):
            down(c, part).start()

    def id_copy(dr):
        to = lax.rem(r + dr, rows)
        return pltpu.make_async_remote_copy(
            table.at[to], ids_v.at[dr], id_send.at[dr], id_recv.at[dr],
            device_id={"row": to}, device_id_type=MESH,
        )

    for dr in range(1, rows):
        id_copy(dr).start()
    ids_v[0] = table[r]
    for load in loads[5:]:
        load.wait()
    bias = jnp.broadcast_to(lb_ref[...], (8, lb_ref.shape[1])).T[:, 0:1]

    def points_one(b, carry):
        points(head_count, b, query_ref, lw_ref, bias, samples_ref, point_s, corner_s, slot_s)
        return carry

    lax.fori_loop(0, local_tiles, points_one, 0)
    index_copy = pltpu.make_async_copy(index_v, index_s, index_sem)
    index_copy.start()
    for dr in range(1, rows):
        id_copy(dr).wait()

    def relay(step, part):
        @pl.when(c - 1 - step >= 0)
        def _():
            block = c - 1 - step
            came_up(block, part).wait_recv()

            @pl.when(c < cols - 1)
            def _():
                up(block, part).start()

        @pl.when(c + 1 + step < cols)
        def _():
            block = c + 1 + step
            came_down(block, part).wait_recv()

            @pl.when(c > 0)
            def _():
                down(block, part).start()

    def row_copy(block, dr, level_num):
        span = spans[level_num]
        first = capacity * sum(spans[:level_num])
        off = rows * first
        size = capacity * span
        return pltpu.make_async_remote_copy(
            stage.at[block, dr - 1, pl.ds(first, size)],
            fetched.at[block, pl.ds(pl.multiple_of(off + r * size, size), size)],
            row_send.at[block, dr, level_num], row_recv.at[block, dr, level_num],
            device_id={"row": lax.rem(r - dr + rows, rows)}, device_id_type=MESH,
        )

    def pick(block):
        for turn in range(rows):
            dr = (turn + 1) % rows
            off = 0
            for level_num in range(LEVELS):
                span = spans[level_num]
                size = capacity * span
                for place in range(capacity):
                    asked = jnp.broadcast_to(
                        ids_v[dr, level_num, pl.ds(block * capacity + place, 1), :], (PACK, lanes_wide)
                    )
                    total = None
                    for tile in range(local_tiles):
                        mask = jnp.where(asked == tile, 1.0, 0.0).astype(jnp.bfloat16)
                        first = local_tiles * off + tile * span
                        part = blocks_v[block, first:first + span, :].reshape(
                            span // PACK, PACK, lanes_wide) * mask[None]
                        total = part if total is None else total + part
                    total = total.reshape(span, lanes_wide)
                    if dr == 0:
                        at = pl.multiple_of(rows * capacity * off + r * size + place * span, span)
                        fetched[block, pl.ds(at, span), :] = total
                    else:
                        at = capacity * off + place * span
                        stage[block, dr - 1, at:at + span, :] = total
                if dr != 0:
                    row_copy(block, dr, level_num).start()
                off += span

    def settle(block):
        for dr in range(1, rows):
            for level_num in range(LEVELS):
                row_copy(block, dr, level_num).wait_recv()

    def weigh(first, last):
        def one(step, carry):
            weigh_block(sides, spans, per_block, head_count, step, point_s, corner_s, slot_s, down_s,
                        spread_s, weight_s)
            return carry

        lax.fori_loop(first, last, one, 0)

    def head_copy(h):
        return pltpu.make_async_remote_copy(
            attn_own.at[h], attn_other.at[h], head_send.at[h], head_recv.at[h],
            device_id={"head": 1 - head}, device_id_type=MESH,
        )

    def keep_sum(h, total):
        mixed[h] = total

    def send_sum(h, total):
        attn_own[h] = total.astype(jnp.bfloat16)
        head_copy(h).start()

    def mix(block, finish=keep_sum):
        settle(block)
        mix_slots(spans, per_block, head_count, head_dim, rows, cols, local_tiles, block, index_s,
                  fetched, turned, keep_s, weight_s, mixed, finish)

    order = group_order(c, cols)
    mixed[...] = jnp.zeros_like(mixed)
    pick(order[0])
    total_steps = local_tiles * head_count
    early = total_steps * 5 // 8
    index_copy.wait()
    for part in range(parts):
        weigh(early * part // parts, early * (part + 1) // parts)
        relay(0, part)
    pick(order[1])
    weigh(early, total_steps)
    for g in range(2, cols):
        for part in range(parts):
            relay(g - 1, part)
            if part == 0:
                mix(order[g - 2])
        pick(order[g])
    mix(order[cols - 2])
    mix(order[cols - 1], send_sum)

    size = mixed.shape[2]
    ch = head_count * head_dim
    own_at = pl.multiple_of(head * ch, ch)
    other_at = pl.multiple_of((1 - head) * ch, ch)
    for h in range(head_count):
        head_copy(h).wait()

    def finish_block(b, carry):
        here = pl.ds(pl.multiple_of(b * head_dim, head_dim), head_dim)
        own = jnp.concatenate([attn_own[h, here, :] for h in range(head_count)], axis=0)
        other = jnp.concatenate([attn_other[h, here, :] for h in range(head_count)], axis=0)

        def project(at):
            lanes = pl.ds(at, ch)
            add = lax.dot_general(
                own, ow_ref[pl.ds(own_at, ch), lanes], (((0,), (0,)), ((), ())),
                preferred_element_type=jnp.float32,
            ) + lax.dot_general(
                other, ow_ref[pl.ds(other_at, ch), lanes], (((0,), (0,)), ((), ())),
                preferred_element_type=jnp.float32,
            )
            return query_ref[b, :, lanes].astype(jnp.float32) + add + ob_ref[:, lanes]

        mine = project(own_at)
        rest = project(other_at)
        scale = 1.0 / (2 * ch)
        mean = jnp.sum(mine + rest, axis=1, keepdims=True) * scale
        mine = mine - mean
        rest = rest - mean
        variance = jnp.sum(mine * mine + rest * rest, axis=1, keepdims=True) * scale
        out_ref[pl.ds(pl.multiple_of(b * size, size), size), :] = mine * lax.rsqrt(variance + 1e-05)
        return carry

    lax.fori_loop(0, local_tiles, finish_block, 0)

    for dr in range(1, rows):
        for block in range(cols):
            for level_num in range(LEVELS):
                row_copy(block, dr, level_num).wait_send()
    for block in range(cols):
        for part in range(parts):
            @pl.when((block <= c) & (c < cols - 1))
            def _(block=block, part=part):
                up(block, part).wait_send()

            @pl.when((block >= c) & (c > 0))
            def _(block=block, part=part):
                down(block, part).wait_send()


def fused_layer(queries, level_blocks, tile_lists, samples, logit_weight, logit_bias, output_weight,
                output_bias, sides, spans):
    rows = lax.axis_size("row")
    cols = lax.axis_size("col")
    tile_rows, tile_cols, level_count, per_block = tile_lists.shape
    local_tiles = tile_rows * tile_cols
    requests = local_tiles * per_block
    channels = level_blocks[0].shape[2]
    lanes = samples.shape[2]
    head_count = lanes // (LEVELS * POINTS)
    head_dim = channels // head_count
    pixels = spans[0]
    tile_span = sum(spans)
    capacity = requests // (rows * cols)
    depth = rows * capacity * tile_span
    flat = [level.reshape(-1, channels) for level in level_blocks[:3]]
    held = (
        tile_lists.reshape(local_tiles, level_count, per_block), level_blocks[3],
        queries.reshape(local_tiles, pixels, queries.shape[2]), logit_weight.T, logit_bias[None, :],
        samples.reshape(local_tiles, pixels, lanes), output_weight, output_bias[None, :],
    )
    vmem = pl.BlockSpec(memory_space=pltpu.VMEM)
    dma = pltpu.SemaphoreType.DMA
    parts = 3
    return pl.pallas_call(
        functools.partial(fused_kernel, sides, spans, per_block, head_count, head_dim, rows, cols),
        out_shape=jax.ShapeDtypeStruct((local_tiles * pixels, channels), jnp.float32),
        in_specs=[pl.BlockSpec(memory_space=pltpu.HBM)] * 11,
        out_specs=vmem,
        scratch_shapes=[
            *[pltpu.VMEM(one.shape, one.dtype) for one in held],
            pltpu.VMEM((cols, local_tiles * tile_span, channels), jnp.bfloat16),
            pltpu.VMEM((rows, LEVELS, requests // rows, channels), jnp.int32),
            pltpu.VMEM((rows, LEVELS, requests // rows, channels), jnp.int32),
            pltpu.VMEM((cols, rows - 1, capacity * tile_span, channels), jnp.bfloat16),
            pltpu.VMEM((cols, depth, channels), jnp.bfloat16),
            pltpu.VMEM((8, 128), jnp.int32),
            pltpu.SMEM((8, 128), jnp.int32),
            pltpu.VMEM((local_tiles, 2, lanes, pixels), jnp.int32),
            pltpu.VMEM((local_tiles, 4, lanes, pixels), jnp.float32),
            pltpu.VMEM((local_tiles, lanes, pixels), jnp.float32),
            pltpu.VMEM((2 * POINTS * PACK, pixels), jnp.float32),
            pltpu.VMEM((POINTS, tile_span, pixels), jnp.bfloat16),
            *[pltpu.VMEM((local_tiles * head_count * per_block, span, pixels), jnp.bfloat16) for span in spans],
            pltpu.VMEM((channels, depth), jnp.bfloat16),
            pltpu.VMEM((local_tiles, PACK, depth), jnp.bfloat16),
            pltpu.VMEM((head_count, local_tiles * head_dim, pixels), jnp.float32),
            pltpu.VMEM((head_count, local_tiles * head_dim, pixels), jnp.bfloat16),
            pltpu.VMEM((head_count, local_tiles * head_dim, pixels), jnp.bfloat16),
            dma((rows,)), dma((rows,)),
            dma((cols, parts)), dma((cols, parts)), dma((cols, parts)), dma((cols, parts)),
            dma((cols, rows, LEVELS)), dma((cols, rows, LEVELS)),
            dma((head_count,)), dma((head_count,)), dma, dma((11,)),
        ],
        compiler_params=pltpu.CompilerParams(
            collective_id=1, has_side_effects=True, vmem_limit_bytes=44 * 1024 * 1024
        ),
        name="fused",
    )(*[pltpu.with_memory_space_constraint(one, pltpu.HBM) for one in (*flat, *held)])


def on_device(
    queries,
    level_zero,
    level_one,
    level_two,
    level_three,
    tile_lists,
    samples,
    logit_weight,
    logit_bias,
    output_weight,
    output_bias,
    norm_gain,
    norm_shift,
):
    level_blocks = (level_zero, level_one, level_two, level_three)
    tile_rows, tile_cols, level_count, per_block = tile_lists.shape
    local_tiles = tile_rows * tile_cols
    requests = local_tiles * per_block
    channels = level_zero.shape[2]
    width_all = queries.shape[2]
    tile_side = level_zero.shape[0] // tile_rows
    pixels = tile_side * tile_side
    sides = [level.shape[0] // tile_rows for level in level_blocks]
    spans = [max(PACK, side * side) for side in sides]
    peer_count = lax.axis_size("row") * lax.axis_size("col")
    full = requests == 2 * peer_count and tile_cols == 1 and sides == [16, 8, 4, 2]
    full = full and all(power_of_two(n) for n in (tile_rows, lax.axis_size("col"), per_block))
    full = full and lax.axis_size("head") == 2 and width_all == 2 * channels
    if full:
        updated = fused_layer(
            queries, level_blocks, tile_lists, samples, logit_weight, logit_bias, output_weight,
            output_bias, sides, spans
        )
        updated = (updated * norm_gain + norm_shift).astype(jnp.bfloat16)
        return updated.reshape(tile_rows * tile_side, tile_cols * tile_side, channels)
    attn_out = gathered_attention(
        queries, level_blocks, tile_lists, samples, logit_weight, logit_bias, sides, spans
    )
    queries_blocked = to_blocks(queries, tile_rows, tile_cols, tile_side)

    head_index = lax.axis_index("head")
    full_attn = lax.all_gather(attn_out, "head", axis=1, tiled=True)
    pre_norm = (
        queries_blocked.reshape(local_tiles * pixels, width_all).astype(jnp.float32)
        + jnp.dot(full_attn, output_weight, preferred_element_type=jnp.float32)
        + output_bias
    )
    row_mean = jnp.mean(pre_norm, axis=1, keepdims=True)
    centered = pre_norm - row_mean
    variance = jnp.mean(centered * centered, axis=1, keepdims=True)
    own_part = lax.dynamic_slice_in_dim(centered, head_index * channels, channels, 1)
    normalized = own_part * lax.rsqrt(variance + 1e-05)
    updated = (normalized * norm_gain + norm_shift).astype(jnp.bfloat16)
    updated = updated.reshape(tile_rows, tile_cols, tile_side, tile_side, channels).transpose(
        0, 2, 1, 3, 4
    )
    return updated.reshape(tile_rows * tile_side, tile_cols * tile_side, channels)


def solution(mesh):
    in_specs = (
        P("row", "col", None),
        P("row", "col", "head"),
        P("row", "col", "head"),
        P("row", "col", "head"),
        P("row", "col", "head"),
        P("row", "col", None, None),
        P("row", "col", "head"),
        P(None, "head"),
        P("head"),
        P(),
        P(),
        P("head"),
        P("head"),
    )
    out_specs = P("row", "col", "head")
    return jax.shard_map(
        on_device, mesh=mesh, in_specs=in_specs, out_specs=out_specs, check_vma=False
    )
```

```python
import functools

import jax
import jax.numpy as jnp
from jax import lax
from jax.experimental import pallas as pl
from jax.experimental.pallas import tpu as pltpu
from jax.sharding import PartitionSpec as P

LEVELS = 4
POINTS = 4
PACK = 16
TURNED = 1
MESH = pl.DeviceIdType.MESH


def to_blocks(source, tile_rows, tile_cols, tile_side):
    channels = source.shape[2]
    shaped = source.reshape(tile_rows, tile_side, tile_cols, tile_side, channels)
    return shaped.transpose(0, 2, 1, 3, 4).reshape(
        tile_rows * tile_cols, tile_side * tile_side, channels
    )


def hat(index, start, low, high):
    return jnp.where(index == start, low, jnp.where(index == start + 1, high, 0.0))


def prepare(head_count, b, query_ref, lw_ref, lb_ref, samples_ref, point_s, corner_s):
    queries_here = query_ref.shape[1]
    hits = LEVELS * POINTS
    logits = lax.dot_general(
        lw_ref[...], query_ref[b], (((1,), (1,)), ((), ())), preferred_element_type=jnp.float32
    ) + lb_ref[...]
    logits = logits.reshape(head_count, hits, queries_here)
    shifted = jnp.exp(logits - jnp.max(logits, axis=1, keepdims=True))
    attend = shifted / jnp.sum(shifted, axis=1, keepdims=True)
    attend = attend.reshape(head_count * hits, queries_here)
    packed = samples_ref[b].T
    pos_row = (packed >> 12) & 4095
    pos_col = packed & 4095
    frac_row = (pos_row & 255).astype(jnp.float32) * (1.0 / 256.0)
    frac_col = (pos_col & 255).astype(jnp.float32) * (1.0 / 256.0)
    point_s[b, 0] = packed >> 24
    point_s[b, 1] = pos_row >> 8
    point_s[b, 2] = pos_col >> 8
    corner_s[b, 0] = attend * (1.0 - frac_row)
    corner_s[b, 1] = attend * frac_row
    corner_s[b, 2] = 1.0 - frac_col
    corner_s[b, 3] = frac_col


def weigh(sides, spans, per_block, b, h, slab, point_s, corner_s, mask_s, weight_s):
    hits = LEVELS * POINTS
    queries_here = weight_s.shape[2]
    lane_row = lax.broadcasted_iota(jnp.int32, (PACK, queries_here), 0)
    slot_row = lax.broadcasted_iota(jnp.int32, (per_block, queries_here), 0)
    level_off = 0
    for level_num in range(LEVELS):
        side = sides[level_num]
        span = spans[level_num]
        rows = [pl.ds(h * hits + level_num * POINTS + p, 1) for p in range(POINTS)]
        for p in range(POINTS):
            mask_s[p * per_block:(p + 1) * per_block, :] = jnp.where(
                slot_row == point_s[b, 0, rows[p], :], 1.0, 0.0
            )
        cols = [
            hat(lane_row % side, point_s[b, 2, rows[p], :], corner_s[b, 2, rows[p], :],
                corner_s[b, 3, rows[p], :])
            for p in range(POINTS)
        ]
        rows_per_chunk = PACK // side

        def chunk(step, carry, rows=rows, cols=cols, side=side, span=span,
                  level_off=level_off, rows_per_chunk=rows_per_chunk):
            parts = []
            for p in range(POINTS):
                index = step * rows_per_chunk
                start = point_s[b, 1, rows[p], :]
                low = corner_s[b, 0, rows[p], :]
                high = corner_s[b, 1, rows[p], :]
                if rows_per_chunk > 1:
                    across = hat(index + lane_row // side, start, low, high)
                else:
                    across = jnp.where(
                        start == index, low, jnp.where(start == index - 1, high, 0.0)
                    )
                parts.append(cols[p] * across)
            for k in range(per_block):
                total = parts[0] * mask_s[k:k + 1, :]
                for p in range(1, POINTS):
                    total = total + parts[p] * mask_s[p * per_block + k:p * per_block + k + 1, :]
                where = pl.multiple_of(level_off + k * span + step * PACK, PACK)
                weight_s[slab, pl.ds(where, PACK), :] = total.astype(jnp.bfloat16)
            return carry

        chunks = span // PACK
        if chunks == 1:
            chunk(0, 0)
        else:
            lax.fori_loop(0, chunks, chunk, 0)
        level_off += span * per_block


def exchange_kernel(sides, spans, per_block, head_count, rows, cols, capacity, local_tiles, *refs):
    (table_ref, tiles_ref, query_ref, lw_ref, lb_ref, samples_ref, fetched_ref, weights_ref) = refs[:8]
    refs = refs[8:]
    held = refs[:cols - 1]
    (ids_v, stage, point_s, corner_s, mask_s, weight_s, id_send, id_recv, col_send, col_recv,
     row_send, row_recv, own_sem, ids_sem, weight_sem) = refs[cols - 1:]
    r = lax.axis_index("row")
    c = lax.axis_index("col")
    lanes_wide = tiles_ref.shape[1]
    barrier = pltpu.get_barrier_semaphore()
    for dc in range(1, cols):
        pl.semaphore_signal(barrier, inc=1, device_id={"col": lax.rem(c + dc, cols)}, device_id_type=MESH)
    for dr in range(1, rows):
        pl.semaphore_signal(barrier, inc=1, device_id={"row": lax.rem(r + dr, rows)}, device_id_type=MESH)
    pl.semaphore_wait(barrier, cols + rows - 2)

    id_copies = []
    for dr in range(1, rows):
        to = lax.rem(r + dr, rows)
        copy = pltpu.make_async_remote_copy(
            table_ref.at[to], ids_v.at[dr], id_send.at[dr], id_recv.at[dr],
            device_id={"row": to}, device_id_type=MESH,
        )
        copy.start()
        id_copies.append(copy)
    col_copies = []
    for dc in range(1, cols):
        copy = pltpu.make_async_remote_copy(
            tiles_ref, held[dc - 1], col_send.at[dc], col_recv.at[dc],
            device_id={"col": lax.rem(c + dc, cols)}, device_id_type=MESH,
        )
        copy.start()
        col_copies.append(copy)
    own_ids = pltpu.make_async_copy(table_ref.at[r], ids_v.at[0], ids_sem)
    own_ids.start()
    own_ids.wait()
    for copy in id_copies:
        copy.wait()

    def pick(dc):
        owner_col = lax.rem(c - dc + cols, cols)
        source = tiles_ref if dc == 0 else held[dc - 1]
        out_at = (r * cols + owner_col) * capacity
        copies = []
        for turn in range(rows):
            dr = (turn + 1) % rows
            for place in range(capacity):
                off = 0
                for level_num in range(LEVELS):
                    span = spans[level_num]
                    at = (owner_col * capacity + place) * LEVELS + level_num
                    asked = jnp.broadcast_to(ids_v[dr, pl.ds(at, 1), :], (PACK, lanes_wide))
                    shape = (span // PACK, PACK, lanes_wide)
                    total = None
                    for tile in range(local_tiles):
                        mask = jnp.where(asked == tile, 1.0, 0.0).astype(jnp.bfloat16)
                        first = local_tiles * off + tile * span
                        part = source[first:first + span, :].reshape(shape) * mask[None]
                        total = part if total is None else total + part
                    stage[dr, dc, place, off:off + span, :] = total.reshape(span, lanes_wide)
                    off += span
            target = fetched_ref.at[pl.ds(out_at, capacity)]
            if dr == 0:
                copy = pltpu.make_async_copy(stage.at[dr, dc], target, own_sem.at[dc])
            else:
                copy = pltpu.make_async_remote_copy(
                    stage.at[dr, dc], target, row_send.at[dr, dc], row_recv.at[dr, dc],
                    device_id={"row": lax.rem(r - dr + rows, rows)}, device_id_type=MESH,
                )
            copy.start()
            copies.append(copy)
        return copies

    copies = pick(0)

    def prepare_one(b, carry):
        prepare(head_count, b, query_ref, lw_ref, lb_ref, samples_ref, point_s, corner_s)
        return carry

    lax.fori_loop(0, local_tiles, prepare_one, 0)

    def store(step, slab):
        return pltpu.make_async_copy(
            weight_s.at[slab], weights_ref.at[step // head_count, step % head_count],
            weight_sem.at[slab],
        )

    def weigh_one(step, carry):
        slab = step % 2

        @pl.when(step >= 2)
        def _():
            store(step - 2, slab).wait()

        weigh(sides, spans, per_block, step // head_count, step % head_count, slab,
              point_s, corner_s, mask_s, weight_s)
        store(step, slab).start()
        return carry

    steps = local_tiles * head_count
    done = 0
    for dc in range(1, cols):
        until = steps * dc // (cols - 1)
        if until > done:
            lax.fori_loop(done, until, weigh_one, 0)
        done = until
        col_copies[dc - 1].wait()
        copies += pick(dc)
    for step in range(max(0, steps - 2), steps):
        store(step, step % 2).wait()
    for copy in copies:
        copy.wait()


def mix_kernel(spans, per_block, head_count, head_dim, pos_ref, fetched_ref, upper_ref, lower_ref,
               out_ref,
               values, values_t, mixed, sem):
    block = pl.program_id(0)
    h = pl.program_id(1)
    blocks = pl.num_programs(0)

    def fetch(which):
        off = 0
        src = 0
        for level_num in range(LEVELS):
            span = spans[level_num]
            for k in range(per_block):
                pltpu.make_async_copy(
                    fetched_ref.at[pos_ref[level_num, which * per_block + k], pl.ds(src, span), :],
                    values.at[which % 2, pl.ds(off, span), :],
                    sem.at[which % 2],
                ).start()
                off += span
            src += span

    @pl.when((h == 0) & (block == 0))
    def _():
        fetch(block)

    @pl.when(h == 0)
    def _():
        side = block % 2
        pltpu.make_async_copy(values.at[side], values.at[side], sem.at[side]).wait()
        values_t[...] = values[side].T.reshape(values_t.shape)

        @pl.when(block + 1 < blocks)
        def _():
            fetch(block + 1)

    half = upper_ref.shape[2]
    mixed[h] = jnp.dot(
        values_t[h, :, :half], upper_ref[0, 0], preferred_element_type=jnp.float32
    ) + jnp.dot(values_t[h, :, half:], lower_ref[0, 0], preferred_element_type=jnp.float32)

    @pl.when(h == head_count - 1)
    def _():
        whole = mixed[...].reshape(head_count * head_dim, mixed.shape[2])
        out_ref[...] = whole.T.astype(jnp.bfloat16)


def gathered_attention(queries, level_blocks, tile_lists, samples, logit_weight, logit_bias, sides, spans):
    row_count = lax.axis_size("row")
    col_count = lax.axis_size("col")
    peer_count = row_count * col_count
    tile_rows, tile_cols, level_count, per_block = tile_lists.shape
    local_tiles = tile_rows * tile_cols
    requests = local_tiles * per_block
    capacity = max(2, (requests + peer_count - 1) // peer_count)
    slots = peer_count * capacity
    grid_cols = tile_cols * col_count
    channels = level_blocks[0].shape[2]
    head_count = samples.shape[2] // (LEVELS * POINTS)
    head_dim = channels // head_count
    tile_side = sides[0]
    pixels = tile_side * tile_side
    tile_span = sum(spans)
    depth = per_block * tile_span

    wanted = tile_lists.transpose(2, 0, 1, 3).reshape(level_count, requests)
    grid_row = wanted // grid_cols
    grid_col = wanted % grid_cols
    owner_dev = grid_row // tile_rows * col_count + grid_col // tile_cols
    local_index = grid_row % tile_rows * tile_cols + grid_col % tile_cols
    order = jnp.arange(requests, dtype=jnp.int32)
    earlier = (owner_dev[:, :, None] == owner_dev[:, None, :]) & (order[None, :] < order[:, None])
    positions = owner_dev * capacity + jnp.sum(earlier.astype(jnp.int32), axis=2)
    slot_order = jnp.arange(slots, dtype=jnp.int32)
    named = positions[:, None, :] == slot_order[None, :, None]
    slot_table = jnp.max(jnp.where(named, local_index[:, None, :], -1), axis=2)
    table = jnp.maximum(slot_table, 0).reshape(level_count, row_count, col_count * capacity)
    table = table.transpose(1, 2, 0).reshape(row_count, col_count * capacity * level_count, 1)
    table_rows = table.shape[1]
    table = jnp.broadcast_to(table, (row_count, table_rows, channels))

    tiles_local = []
    for level_num in range(level_count):
        tiles = to_blocks(level_blocks[level_num], tile_rows, tile_cols, sides[level_num])
        short = spans[level_num] - tiles.shape[1]
        if short > 0:
            tiles = jnp.pad(tiles, ((0, 0), (0, short), (0, 0)))
        tiles_local.append(tiles.reshape(local_tiles * spans[level_num], channels))
    tiles_local = jnp.concatenate(tiles_local, axis=0)

    queries_blocked = to_blocks(queries, tile_rows, tile_cols, tile_side)
    samples_blocked = to_blocks(samples, tile_rows, tile_cols, tile_side)
    lanes = head_count * LEVELS * POINTS
    vmem = pl.BlockSpec(memory_space=pltpu.VMEM)
    whole = pl.BlockSpec(memory_space=pl.ANY)
    dma = pltpu.SemaphoreType.DMA
    fetched, weights = pl.pallas_call(
        functools.partial(exchange_kernel, sides, spans, per_block, head_count, row_count,
                          col_count, capacity, local_tiles),
        out_shape=(
            jax.ShapeDtypeStruct((slots, tile_span, channels), jnp.bfloat16),
            jax.ShapeDtypeStruct((local_tiles, head_count, depth, pixels), jnp.bfloat16),
        ),
        in_specs=[vmem] * 6,
        out_specs=(whole, whole),
        scratch_shapes=[
            pltpu.VMEM((local_tiles * tile_span, channels), jnp.bfloat16)
            for _ in range(col_count - 1)
        ] + [
            pltpu.VMEM((row_count, table_rows, channels), jnp.int32),
            pltpu.VMEM((row_count, col_count, capacity, tile_span, channels), jnp.bfloat16),
            pltpu.VMEM((local_tiles, 3, lanes, pixels), jnp.int32),
            pltpu.VMEM((local_tiles, 4, lanes, pixels), jnp.float32),
            pltpu.VMEM((POINTS * per_block, pixels), jnp.float32),
            pltpu.VMEM((2, depth, pixels), jnp.bfloat16),
            dma((row_count,)), dma((row_count,)), dma((col_count,)), dma((col_count,)),
            dma((row_count, col_count)), dma((row_count, col_count)), dma((col_count,)),
            dma, dma((2,)),
        ],
        compiler_params=pltpu.CompilerParams(
            collective_id=0, has_side_effects=True, vmem_limit_bytes=60 * 1024 * 1024
        ),
        cost_estimate=pl.CostEstimate(
            flops=8 * local_tiles * head_count * depth * pixels * POINTS,
            bytes_accessed=2 * local_tiles * head_count * depth * pixels, transcendentals=0,
        ),
        name="exchange",
    )(table, tiles_local, queries_blocked, logit_weight.T, logit_bias[:, None], samples_blocked)

    attn_out = pl.pallas_call(
        functools.partial(mix_kernel, spans, per_block, head_count, head_dim),
        grid_spec=pltpu.PrefetchScalarGridSpec(
            num_scalar_prefetch=1,
            grid=(local_tiles, head_count),
            in_specs=[
                pl.BlockSpec(memory_space=pl.ANY),
                pl.BlockSpec((1, 1, depth // 2, pixels), lambda b, h, pos: (b, h, 0, 0)),
                pl.BlockSpec((1, 1, depth // 2, pixels), lambda b, h, pos: (b, h, 1, 0)),
            ],
            out_specs=pl.BlockSpec((pixels, channels), lambda b, h, pos: (b, 0)),
            scratch_shapes=[
                pltpu.VMEM((2, depth, channels), jnp.bfloat16),
                pltpu.VMEM((head_count, head_dim, depth), jnp.bfloat16),
                pltpu.VMEM((head_count, head_dim, pixels), jnp.float32),
                pltpu.SemaphoreType.DMA((2,)),
            ],
        ),
        out_shape=jax.ShapeDtypeStruct((local_tiles * pixels, channels), jnp.bfloat16),
        compiler_params=pltpu.CompilerParams(
            dimension_semantics=("arbitrary", "arbitrary"), vmem_limit_bytes=60 * 1024 * 1024
        ),
        cost_estimate=pl.CostEstimate(
            flops=2 * local_tiles * depth * pixels * channels,
            bytes_accessed=2 * local_tiles * head_count * depth * pixels, transcendentals=0,
        ),
        name="mix",
    )(positions, fetched, weights, weights)
    return attn_out


def power_of_two(n):
    return n > 0 and n & (n - 1) == 0


def group_order(c, cols):
    near = jnp.minimum(c, cols - 1 - c)
    order = [c]
    for g in range(1, cols):
        both = c - (g + 1) // 2 if g % 2 else c + g // 2
        one = jnp.where(c < cols - 1 - c, c + g - near, c - g + near)
        order.append(jnp.where(g <= 2 * near, both, one))
    return order


def plan_tables(rows, cols, per_block, lists_ref, table, turned_table, index_v):
    blocks = lists_ref.shape[0]
    wanted = jnp.concatenate([lists_ref[b] for b in range(blocks)], axis=1)
    requests = wanted.shape[1]
    tile_rows = blocks
    col_bits = cols.bit_length() - 1
    row_bits = tile_rows.bit_length() - 1
    shape = (requests, requests)
    down = lax.broadcasted_iota(jnp.int32, shape, 0)
    along = lax.broadcasted_iota(jnp.int32, shape, 1)
    capacity = requests // (rows * cols)
    for level_num in range(LEVELS):
        here = jnp.broadcast_to(wanted[level_num:level_num + 1, :], shape)
        if level_num == TURNED:
            own_here = (here & (cols - 1)) * rows + (here >> (col_bits + row_bits))
        else:
            own_here = ((here >> (col_bits + row_bits)) << col_bits) + (here & (cols - 1))
        local_here = (here >> col_bits) & (tile_rows - 1)
        same = own_here == own_here.T
        place_here = jnp.sum(jnp.where(same & (down < along), 1, 0), axis=0, keepdims=True)
        slot_here = own_here * capacity + place_here
        asked = jnp.sum(
            jnp.where(slot_here == down, local_here.astype(jnp.float32), 0.0), axis=1, keepdims=True
        )
        asked = jnp.broadcast_to(asked, (requests, table.shape[3])).astype(jnp.int32)
        if level_num == TURNED:
            turned_table[...] = asked.reshape(turned_table.shape)
        else:
            table[:, level_num] = asked.reshape(rows, requests // rows, table.shape[3])
        filled = jnp.sum(jnp.where(slot_here.T == along, down, 0), axis=0, keepdims=True)
        index_v[level_num:level_num + 1, 0:requests] = filled


def points(head_count, b, query_ref, lw_ref, bias, samples_ref, point_s, corner_s, slot_s):
    queries_here = query_ref.shape[1]
    hits = LEVELS * POINTS
    logits = lax.dot_general(
        lw_ref[...], query_ref[b], (((1,), (1,)), ((), ())), preferred_element_type=jnp.float32
    ) + bias
    logits = logits.reshape(head_count, hits, queries_here)
    shifted = jnp.exp(logits - jnp.max(logits, axis=1, keepdims=True))
    attend = shifted / jnp.sum(shifted, axis=1, keepdims=True)
    attend = attend.reshape(head_count * hits, queries_here)
    packed = samples_ref[b].T
    pos_row = (packed >> 12) & 4095
    pos_col = packed & 4095
    frac_row = (pos_row & 255).astype(jnp.float32) * (1.0 / 256.0)
    frac_col = (pos_col & 255).astype(jnp.float32) * (1.0 / 256.0)
    point_s[b, 0] = pos_row >> 8
    point_s[b, 1] = pos_col >> 8
    corner_s[b, 0] = attend * (1.0 - frac_row)
    corner_s[b, 1] = attend * frac_row
    corner_s[b, 2] = 1.0 - frac_col
    corner_s[b, 3] = frac_col
    slot_s[b] = (packed >> 24).astype(jnp.float32)


def hats(start, low, high, count):
    here = [start == i for i in range(count)]
    out = [jnp.where(here[0], low, 0.0)]
    for i in range(1, count):
        out.append(jnp.where(here[i], low, jnp.where(here[i - 1], high, 0.0)))
    return out


def weigh_block(sides, spans, per_block, head_count, step, point_s, corner_s, slot_s, down_s, spread_s,
                weight_s):
    hits = LEVELS * POINTS
    queries_here = spread_s.shape[2]
    b = step // head_count
    h = step % head_count
    half = PACK // 2
    lane_row = lax.broadcasted_iota(jnp.int32, (PACK, queries_here), 0)
    off = 0
    for level_num in range(LEVELS):
        side = sides[level_num]
        span = spans[level_num]
        for p in range(POINTS):
            row = pl.ds(h * hits + level_num * POINTS + p, 1)
            across = hat(lane_row % side, point_s[b, 1, row, :], corner_s[b, 2, row, :],
                         corner_s[b, 3, row, :])
            down = hat(lane_row // side if side < half else lane_row, point_s[b, 0, row, :],
                       corner_s[b, 0, row, :], corner_s[b, 1, row, :])
            if side >= half:
                at_down = (level_num * POINTS + p) * PACK
                down_s[at_down:at_down + PACK, :] = down
                for chunk in range(span // PACK):
                    parts = []
                    for part in range(2):
                        at = chunk * PACK + part * half
                        col = at % side if side > half else part * half
                        line = at_down + at // side
                        parts.append(across[col:col + half, :] * down_s[line:line + 1, :])
                    total = jnp.concatenate(parts, axis=0).astype(jnp.bfloat16)
                    spread_s[p, off + chunk * PACK:off + (chunk + 1) * PACK, :] = total
            else:
                spread_s[p, off:off + PACK, :] = (across * down).astype(jnp.bfloat16)
        off += span
    off = 0
    quad = 4
    one = jnp.ones((PACK, queries_here), jnp.bfloat16)
    none = jnp.zeros((PACK, queries_here), jnp.bfloat16)
    for level_num in range(LEVELS):
        span = spans[level_num]
        slots = []
        for p in range(POINTS):
            mine = slot_s[b, pl.ds(h * hits + level_num * POINTS + p, 1), :]
            slots.append(jnp.broadcast_to(mine, (PACK, queries_here)).astype(jnp.bfloat16))
        for first in range(0, per_block, quad):
            masks = []
            for k in range(first, first + quad):
                label = jnp.full((PACK, queries_here), k, jnp.bfloat16)
                masks.append([jnp.where(slots[p] == label, one, none) for p in range(POINTS)])
            for chunk in range(span // PACK):
                pieces = [spread_s[p, off + chunk * PACK:off + (chunk + 1) * PACK, :] for p in range(POINTS)]
                for k in range(first, first + quad):
                    total = pieces[0] * masks[k - first][0]
                    for p in range(1, POINTS):
                        total = total + pieces[p] * masks[k - first][p]
                    weight_s[level_num][step * per_block + k, chunk * PACK:(chunk + 1) * PACK, :] = total
        off += span


def mix_slots(spans, per_block, head_count, head_dim, rows, cols, blocks, pieces, index_s, fetched,
              turned, keep_s, weight_s, mixed, finish):
    capacity = 2
    units = rows * capacity
    lanes = 128
    block_bits = per_block.bit_length() - 1
    requests = blocks * per_block
    lane = lax.broadcasted_iota(jnp.int32, (1, lanes), 1)

    def entry_of(group, level_num, unit):
        if level_num == TURNED:
            slot = group * units + unit
        else:
            slot = (unit // capacity * cols + group) * capacity + unit % capacity
        return index_s[level_num, slot] & (requests - 1)

    owners = []
    depth = 0
    for group, level_num in pieces:
        span = spans[level_num]
        size = units * span
        at = units * sum(spans[:level_num])
        turned[:, depth:depth + size] = fetched[group, at:at + size, :].T
        depth += size
        block_of = [entry_of(group, level_num, unit) >> block_bits for unit in range(units)]
        for start in range(0, size, lanes):
            first = start // span
            last = (start + lanes - 1) // span
            value = jnp.full((1, lanes), block_of[first], jnp.int32)
            for unit in range(first + 1, last + 1):
                value = jnp.where(lane >= unit * span - start, block_of[unit], value)
            owners.append(value)
    owner_row = jnp.concatenate(owners, axis=1)
    for b in range(blocks):
        keep_s[b, :, 0:depth] = jnp.broadcast_to(
            jnp.where(owner_row == b, 1.0, 0.0), (PACK, depth)
        ).astype(jnp.bfloat16)

    def one_head(h, carry):
        left = jnp.concatenate([
            turned[pl.ds(pl.multiple_of(h * head_dim + half, PACK), PACK), 0:depth]
            * keep_s[b, :, 0:depth]
            for b in range(blocks) for half in range(0, head_dim, PACK)
        ], axis=0)
        right = []
        for group, level_num in pieces:
            for unit in range(units):
                entry = entry_of(group, level_num, unit)
                source = (entry >> block_bits) * head_count + h
                right.append(weight_s[level_num][source * per_block + (entry & (per_block - 1))])
        right = jnp.concatenate(right, axis=0)
        total = mixed[h] + jnp.dot(left, right, preferred_element_type=jnp.float32)
        finish(h, total)
        return carry

    lax.fori_loop(0, head_count, one_head, 0)


def fused_kernel(sides, spans, per_block, head_count, head_dim, rows, cols, *refs):
    sources, refs = refs[:11], refs[11:]
    out_ref, refs = refs[0], refs[1:]
    held, refs = refs[:8], refs[8:]
    (lists_ref, three_ref, query_ref, lw_ref, lb_ref, samples_ref, ow_ref, ob_ref) = held
    (layer_v, turned_table, turned_ids, turned_stage, blocks_v, table, ids_v, stage, fetched, index_v, index_s, point_s,
     corner_s, slot_s, down_s, spread_s, weight_0, weight_1, weight_2, weight_3, turned, keep_s, mixed,
     attn_own, attn_other, id_send, id_recv, up_send, up_recv, down_send, down_recv, row_send, row_recv,
     head_send, head_recv, layer_send, layer_recv, list_send, list_recv, turned_send, turned_recv,
     index_sem, in_sem) = refs
    weight_s = (weight_0, weight_1, weight_2, weight_3)
    local_tiles = lists_ref.shape[0]
    capacity = 2
    r = lax.axis_index("row")
    c = lax.axis_index("col")
    head = lax.axis_index("head")
    lanes_wide = blocks_v.shape[2]
    starts = {}
    off = 0
    for level_num in range(LEVELS):
        if level_num != TURNED:
            starts[level_num] = off
            off += local_tiles * spans[level_num]
    targets = [
        layer_v.at[r] if level_num == TURNED
        else blocks_v.at[c, pl.ds(starts[level_num], local_tiles * spans[level_num])]
        for level_num in range(3)
    ]
    loads = [
        pltpu.make_async_copy(source, target, in_sem.at[i])
        for i, (source, target) in enumerate(zip(sources, targets + list(held)))
    ]
    for load in loads:
        load.start()
    barrier = pltpu.get_barrier_semaphore()
    pl.semaphore_signal(barrier, inc=1, device_id={"head": 1 - head}, device_id_type=MESH)
    for dr in range(1, rows):
        pl.semaphore_signal(barrier, inc=1, device_id={"row": lax.rem(r + dr, rows)}, device_id_type=MESH)
    for dc in range(1, cols):
        pl.semaphore_signal(barrier, inc=1, device_id={"col": lax.rem(c + dc, cols)}, device_id_type=MESH)
    for load in loads[3:5]:
        load.wait()
    span = spans[3]
    side = sides[3]
    for tile in range(local_tiles):
        rows_here = jnp.concatenate(
            [three_ref[tile * side + i].astype(jnp.float32) for i in range(side)]
            + [jnp.zeros((span - side * side, lanes_wide), jnp.float32)], axis=0
        )
        at = starts[3] + tile * span
        blocks_v[c, at:at + span, :] = rows_here.astype(jnp.bfloat16)
    plan_tables(rows, cols, per_block, lists_ref, table, turned_table, index_v)

    for load in loads[:3]:
        load.wait()
    pl.semaphore_wait(barrier, rows + cols - 1)

    block_rows = blocks_v.shape[1]
    parts = 3
    part_rows = block_rows // parts

    def up(block, part):
        at = blocks_v.at[block, pl.ds(pl.multiple_of(part * part_rows, PACK), part_rows)]
        return pltpu.make_async_remote_copy(
            at, at, up_send.at[c - block, part], up_recv.at[c - block, part],
            device_id={"col": c + 1}, device_id_type=MESH,
        )

    def down(block, part):
        at = blocks_v.at[block, pl.ds(pl.multiple_of(part * part_rows, PACK), part_rows)]
        return pltpu.make_async_remote_copy(
            at, at, down_send.at[block - c, part], down_recv.at[block - c, part],
            device_id={"col": c - 1}, device_id_type=MESH,
        )

    def came_up(block, part):
        at = blocks_v.at[block, pl.ds(pl.multiple_of(part * part_rows, PACK), part_rows)]
        return pltpu.make_async_remote_copy(
            at, at, up_send.at[c - 1 - block, part], up_recv.at[c - 1 - block, part],
            device_id={"col": c - 1}, device_id_type=MESH,
        )

    def came_down(block, part):
        at = blocks_v.at[block, pl.ds(pl.multiple_of(part * part_rows, PACK), part_rows)]
        return pltpu.make_async_remote_copy(
            at, at, down_send.at[block - c - 1, part], down_recv.at[block - c - 1, part],
            device_id={"col": c + 1}, device_id_type=MESH,
        )

    def id_copy(dr):
        to = lax.rem(r + dr, rows)
        return pltpu.make_async_remote_copy(
            table.at[to], ids_v.at[dr], id_send.at[dr], id_recv.at[dr],
            device_id={"row": to}, device_id_type=MESH,
        )

    def list_copy(dc):
        to = lax.rem(c + dc, cols)
        return pltpu.make_async_remote_copy(
            turned_table.at[to], turned_ids.at[c], list_send.at[dc], list_recv.at[dc],
            device_id={"col": to}, device_id_type=MESH,
        )

    def layer_copy(dr):
        return pltpu.make_async_remote_copy(
            layer_v.at[r], layer_v.at[r], layer_send.at[dr], layer_recv.at[dr],
            device_id={"row": lax.rem(r + dr, rows)}, device_id_type=MESH,
        )

    def layer_came(dr):
        at = layer_v.at[lax.rem(r - dr + rows, rows)]
        return pltpu.make_async_remote_copy(
            at, at, layer_send.at[dr], layer_recv.at[dr],
            device_id={"row": lax.rem(r + dr, rows)}, device_id_type=MESH,
        )

    def list_came(dc):
        return pltpu.make_async_remote_copy(
            turned_table.at[c], turned_ids.at[lax.rem(c - dc + cols, cols)], list_send.at[dc],
            list_recv.at[dc], device_id={"col": lax.rem(c + dc, cols)}, device_id_type=MESH,
        )

    for dr in range(1, rows):
        id_copy(dr).start()
    for dc in range(1, cols):
        list_copy(dc).start()
    for part in range(parts):
        @pl.when(c < cols - 1)
        def _(part=part):
            up(c, part).start()

        @pl.when(c > 0)
        def _(part=part):
            down(c, part).start()

    for dr in range(1, rows):
        layer_copy(dr).start()
    turned_ids[c] = turned_table[c]
    ids_v[0] = table[r]
    for load in loads[5:]:
        load.wait()
    bias = jnp.broadcast_to(lb_ref[...], (8, lb_ref.shape[1])).T[:, 0:1]

    def points_one(b, carry):
        points(head_count, b, query_ref, lw_ref, bias, samples_ref, point_s, corner_s, slot_s)
        return carry

    lax.fori_loop(0, local_tiles, points_one, 0)
    index_copy = pltpu.make_async_copy(index_v, index_s, index_sem)
    index_copy.start()
    for dr in range(1, rows):
        id_copy(dr).wait()

    def relay(step, part):
        @pl.when(c - 1 - step >= 0)
        def _():
            block = c - 1 - step
            came_up(block, part).wait_recv()

            @pl.when(c < cols - 1)
            def _():
                up(block, part).start()

        @pl.when(c + 1 + step < cols)
        def _():
            block = c + 1 + step
            came_down(block, part).wait_recv()

            @pl.when(c > 0)
            def _():
                down(block, part).start()

    def row_copy(block, dr, level_num):
        span = spans[level_num]
        first = capacity * sum(spans[:level_num])
        off = rows * first
        size = capacity * span
        return pltpu.make_async_remote_copy(
            stage.at[block, dr - 1, pl.ds(first, size)],
            fetched.at[block, pl.ds(pl.multiple_of(off + r * size, size), size)],
            row_send.at[block, dr, level_num], row_recv.at[block, dr, level_num],
            device_id={"row": lax.rem(r - dr + rows, rows)}, device_id_type=MESH,
        )

    def pick(block):
        for turn in range(rows):
            dr = (turn + 1) % rows
            off = 0
            for level_num in range(LEVELS):
                span = spans[level_num]
                size = capacity * span
                if level_num == TURNED:
                    off += span
                    continue
                for place in range(capacity):
                    asked = jnp.broadcast_to(
                        ids_v[dr, level_num, pl.ds(block * capacity + place, 1), :], (PACK, lanes_wide)
                    )
                    total = None
                    for tile in range(local_tiles):
                        mask = jnp.where(asked == tile, 1.0, 0.0).astype(jnp.bfloat16)
                        first = starts[level_num] + tile * span
                        part = blocks_v[block, first:first + span, :].reshape(
                            span // PACK, PACK, lanes_wide) * mask[None]
                        total = part if total is None else total + part
                    total = total.reshape(span, lanes_wide)
                    if dr == 0:
                        at = pl.multiple_of(rows * capacity * off + r * size + place * span, span)
                        fetched[block, pl.ds(at, span), :] = total
                    else:
                        at = capacity * off + place * span
                        stage[block, dr - 1, at:at + span, :] = total
                if dr != 0:
                    row_copy(block, dr, level_num).start()
                off += span

    turned_span = spans[TURNED]
    turned_at = rows * capacity * sum(spans[:TURNED])
    turned_size = rows * capacity * turned_span

    def turned_copy(block, to):
        return pltpu.make_async_remote_copy(
            turned_stage.at[to], fetched.at[block, pl.ds(turned_at, turned_size)],
            turned_send.at[to], turned_recv.at[block],
            device_id={"col": to}, device_id_type=MESH,
        )

    def pick_turned(to, target, base):
        for owner in range(rows):
            for place in range(capacity):
                unit = owner * capacity + place
                asked = jnp.broadcast_to(turned_ids[to, pl.ds(unit, 1), :], (PACK, lanes_wide))
                total = None
                for tile in range(local_tiles):
                    mask = jnp.where(asked == tile, 1.0, 0.0).astype(jnp.bfloat16)
                    part = layer_v[owner, tile * turned_span:(tile + 1) * turned_span, :].reshape(
                        turned_span // PACK, PACK, lanes_wide) * mask[None]
                    total = part if total is None else total + part
                at = base + unit * turned_span
                target[at:at + turned_span, :] = total.reshape(turned_span, lanes_wide)

    def send_turned(step):
        for to, before in ((step + 1, True), (cols - 2 - step, False)):
            @pl.when(c < to if before else c > to)
            def _(to=to):
                pick_turned(to, turned_stage.at[to], 0)
                turned_copy(c, to).start()

    def settle(block):
        for dr in range(1, rows):
            for level_num in range(LEVELS):
                if level_num != TURNED:
                    row_copy(block, dr, level_num).wait_recv()

    def weigh(first, last):
        def one(step, carry):
            weigh_block(sides, spans, per_block, head_count, step, point_s, corner_s, slot_s, down_s,
                        spread_s, weight_s)
            return carry

        lax.fori_loop(first, last, one, 0)

    def head_copy(h):
        return pltpu.make_async_remote_copy(
            attn_own.at[h], attn_other.at[h], head_send.at[h], head_recv.at[h],
            device_id={"head": 1 - head}, device_id_type=MESH,
        )

    def keep_sum(h, total):
        mixed[h] = total

    def send_sum(h, total):
        attn_own[h] = total.astype(jnp.bfloat16)
        head_copy(h).start()

    straight = [level_num for level_num in range(LEVELS) if level_num != TURNED]

    def mix(pieces, finish=keep_sum):
        mix_slots(spans, per_block, head_count, head_dim, rows, cols, local_tiles, pieces, index_s,
                  fetched, turned, keep_s, weight_s, mixed, finish)

    def mix_straight(block, finish=keep_sum):
        settle(block)
        mix([(block, level_num) for level_num in straight], finish)

    order = group_order(c, cols)
    mixed[...] = jnp.zeros_like(mixed)
    pick(order[0])
    total_steps = local_tiles * head_count
    index_copy.wait()

    def relay_and_weigh(step, share):
        def one(part, carry):
            first = (step * parts + part) * share
            weigh(jnp.minimum(first, total_steps), jnp.minimum(first + share, total_steps))
            relay(step, part)
            return carry

        lax.fori_loop(0, parts, one, 0)

    for g in range(1, cols):
        relay_and_weigh(g - 1, -(-total_steps // (parts * (cols - 1))))
        pick(order[g])
        if g == 1:
            for dr in range(1, rows):
                layer_came(dr).wait_recv()
            for dc in range(1, cols):
                list_came(dc).wait_recv()
            pick_turned(c, fetched.at[c], turned_at)
        send_turned(g - 1)
    settle(order[0])
    mix([(order[0], level_num) for level_num in range(LEVELS)])
    for g in range(1, cols - 1):
        mix_straight(order[g])
    for g in range(1, cols):
        turned_copy(order[g], order[g]).wait_recv()
    mix([(order[g], TURNED) for g in range(1, cols)])
    mix_straight(order[cols - 1], send_sum)

    size = mixed.shape[2]
    ch = head_count * head_dim
    own_at = pl.multiple_of(head * ch, ch)
    other_at = pl.multiple_of((1 - head) * ch, ch)
    for h in range(head_count):
        head_copy(h).wait()

    def finish_block(b, carry):
        here = pl.ds(pl.multiple_of(b * head_dim, head_dim), head_dim)
        own = jnp.concatenate([attn_own[h, here, :] for h in range(head_count)], axis=0)
        other = jnp.concatenate([attn_other[h, here, :] for h in range(head_count)], axis=0)

        def project(at):
            lanes = pl.ds(at, ch)
            add = lax.dot_general(
                own, ow_ref[pl.ds(own_at, ch), lanes], (((0,), (0,)), ((), ())),
                preferred_element_type=jnp.float32,
            ) + lax.dot_general(
                other, ow_ref[pl.ds(other_at, ch), lanes], (((0,), (0,)), ((), ())),
                preferred_element_type=jnp.float32,
            )
            return query_ref[b, :, lanes].astype(jnp.float32) + add + ob_ref[:, lanes]

        mine = project(own_at)
        rest = project(other_at)
        scale = 1.0 / (2 * ch)
        mean = jnp.sum(mine + rest, axis=1, keepdims=True) * scale
        mine = mine - mean
        rest = rest - mean
        variance = jnp.sum(mine * mine + rest * rest, axis=1, keepdims=True) * scale
        out_ref[pl.ds(pl.multiple_of(b * size, size), size), :] = mine * lax.rsqrt(variance + 1e-05)
        return carry

    lax.fori_loop(0, local_tiles, finish_block, 0)

    for dr in range(1, rows):
        layer_copy(dr).wait_send()
        for block in range(cols):
            for level_num in range(LEVELS):
                if level_num != TURNED:
                    row_copy(block, dr, level_num).wait_send()
    for dc in range(1, cols):
        list_copy(dc).wait_send()
        turned_copy(c, lax.rem(c + dc, cols)).wait_send()
    for block in range(cols):
        for part in range(parts):
            @pl.when((block <= c) & (c < cols - 1))
            def _(block=block, part=part):
                up(block, part).wait_send()

            @pl.when((block >= c) & (c > 0))
            def _(block=block, part=part):
                down(block, part).wait_send()


def fused_layer(queries, level_blocks, tile_lists, samples, logit_weight, logit_bias, output_weight,
                output_bias, sides, spans):
    rows = lax.axis_size("row")
    cols = lax.axis_size("col")
    tile_rows, tile_cols, level_count, per_block = tile_lists.shape
    local_tiles = tile_rows * tile_cols
    requests = local_tiles * per_block
    channels = level_blocks[0].shape[2]
    lanes = samples.shape[2]
    head_count = lanes // (LEVELS * POINTS)
    head_dim = channels // head_count
    pixels = spans[0]
    tile_span = sum(spans)
    capacity = requests // (rows * cols)
    depth = rows * capacity * tile_span
    flat = [level.reshape(-1, channels) for level in level_blocks[:3]]
    held = (
        tile_lists.reshape(local_tiles, level_count, per_block), level_blocks[3],
        queries.reshape(local_tiles, pixels, queries.shape[2]), logit_weight.T, logit_bias[None, :],
        samples.reshape(local_tiles, pixels, lanes), output_weight, output_bias[None, :],
    )
    vmem = pl.BlockSpec(memory_space=pltpu.VMEM)
    dma = pltpu.SemaphoreType.DMA
    parts = 3
    return pl.pallas_call(
        functools.partial(fused_kernel, sides, spans, per_block, head_count, head_dim, rows, cols),
        out_shape=jax.ShapeDtypeStruct((local_tiles * pixels, channels), jnp.float32),
        in_specs=[pl.BlockSpec(memory_space=pltpu.HBM)] * 11,
        out_specs=vmem,
        scratch_shapes=[
            *[pltpu.VMEM(one.shape, one.dtype) for one in held],
            pltpu.VMEM((rows, local_tiles * spans[TURNED], channels), jnp.bfloat16),
            pltpu.VMEM((cols, requests // cols, channels), jnp.int32),
            pltpu.VMEM((cols, requests // cols, channels), jnp.int32),
            pltpu.VMEM((cols, rows * capacity * spans[TURNED], channels), jnp.bfloat16),
            pltpu.VMEM((cols, local_tiles * (tile_span - spans[TURNED]), channels), jnp.bfloat16),
            pltpu.VMEM((rows, LEVELS, requests // rows, channels), jnp.int32),
            pltpu.VMEM((rows, LEVELS, requests // rows, channels), jnp.int32),
            pltpu.VMEM((cols, rows - 1, capacity * tile_span, channels), jnp.bfloat16),
            pltpu.VMEM((cols, depth, channels), jnp.bfloat16),
            pltpu.VMEM((8, 128), jnp.int32),
            pltpu.SMEM((8, 128), jnp.int32),
            pltpu.VMEM((local_tiles, 2, lanes, pixels), jnp.int32),
            pltpu.VMEM((local_tiles, 4, lanes, pixels), jnp.float32),
            pltpu.VMEM((local_tiles, lanes, pixels), jnp.float32),
            pltpu.VMEM((2 * POINTS * PACK, pixels), jnp.float32),
            pltpu.VMEM((POINTS, tile_span, pixels), jnp.bfloat16),
            *[pltpu.VMEM((local_tiles * head_count * per_block, span, pixels), jnp.bfloat16) for span in spans],
            pltpu.VMEM((channels, depth), jnp.bfloat16),
            pltpu.VMEM((local_tiles, PACK, depth), jnp.bfloat16),
            pltpu.VMEM((head_count, local_tiles * head_dim, pixels), jnp.float32),
            pltpu.VMEM((head_count, local_tiles * head_dim, pixels), jnp.bfloat16),
            pltpu.VMEM((head_count, local_tiles * head_dim, pixels), jnp.bfloat16),
            dma((rows,)), dma((rows,)),
            dma((cols, parts)), dma((cols, parts)), dma((cols, parts)), dma((cols, parts)),
            dma((cols, rows, LEVELS)), dma((cols, rows, LEVELS)),
            dma((head_count,)), dma((head_count,)), dma((rows,)), dma((rows,)),
            dma((cols,)), dma((cols,)), dma((cols,)), dma((cols,)), dma, dma((11,)),
        ],
        compiler_params=pltpu.CompilerParams(
            collective_id=1, has_side_effects=True, vmem_limit_bytes=44 * 1024 * 1024
        ),
        name="fused",
    )(*[pltpu.with_memory_space_constraint(one, pltpu.HBM) for one in (*flat, *held)])


def on_device(
    queries,
    level_zero,
    level_one,
    level_two,
    level_three,
    tile_lists,
    samples,
    logit_weight,
    logit_bias,
    output_weight,
    output_bias,
    norm_gain,
    norm_shift,
):
    level_blocks = (level_zero, level_one, level_two, level_three)
    tile_rows, tile_cols, level_count, per_block = tile_lists.shape
    local_tiles = tile_rows * tile_cols
    requests = local_tiles * per_block
    channels = level_zero.shape[2]
    width_all = queries.shape[2]
    tile_side = level_zero.shape[0] // tile_rows
    pixels = tile_side * tile_side
    sides = [level.shape[0] // tile_rows for level in level_blocks]
    spans = [max(PACK, side * side) for side in sides]
    peer_count = lax.axis_size("row") * lax.axis_size("col")
    full = requests == 2 * peer_count and tile_cols == 1 and sides == [16, 8, 4, 2]
    full = full and all(power_of_two(n) for n in (tile_rows, lax.axis_size("col"), per_block))
    full = full and lax.axis_size("head") == 2 and width_all == 2 * channels
    if full:
        updated = fused_layer(
            queries, level_blocks, tile_lists, samples, logit_weight, logit_bias, output_weight,
            output_bias, sides, spans
        )
        updated = (updated * norm_gain + norm_shift).astype(jnp.bfloat16)
        return updated.reshape(tile_rows * tile_side, tile_cols * tile_side, channels)
    attn_out = gathered_attention(
        queries, level_blocks, tile_lists, samples, logit_weight, logit_bias, sides, spans
    )
    queries_blocked = to_blocks(queries, tile_rows, tile_cols, tile_side)

    head_index = lax.axis_index("head")
    full_attn = lax.all_gather(attn_out, "head", axis=1, tiled=True)
    pre_norm = (
        queries_blocked.reshape(local_tiles * pixels, width_all).astype(jnp.float32)
        + jnp.dot(full_attn, output_weight, preferred_element_type=jnp.float32)
        + output_bias
    )
    row_mean = jnp.mean(pre_norm, axis=1, keepdims=True)
    centered = pre_norm - row_mean
    variance = jnp.mean(centered * centered, axis=1, keepdims=True)
    own_part = lax.dynamic_slice_in_dim(centered, head_index * channels, channels, 1)
    normalized = own_part * lax.rsqrt(variance + 1e-05)
    updated = (normalized * norm_gain + norm_shift).astype(jnp.bfloat16)
    updated = updated.reshape(tile_rows, tile_cols, tile_side, tile_side, channels).transpose(
        0, 2, 1, 3, 4
    )
    return updated.reshape(tile_rows * tile_side, tile_cols * tile_side, channels)


def solution(mesh):
    in_specs = (
        P("row", "col", None),
        P("row", "col", "head"),
        P("row", "col", "head"),
        P("row", "col", "head"),
        P("row", "col", "head"),
        P("row", "col", None, None),
        P("row", "col", "head"),
        P(None, "head"),
        P("head"),
        P(),
        P(),
        P("head"),
        P("head"),
    )
    out_specs = P("row", "col", "head")
    return jax.shard_map(
        on_device, mesh=mesh, in_specs=in_specs, out_specs=out_specs, check_vma=False
    )
```

```python
import functools

import jax
import jax.numpy as jnp
from jax import lax
from jax.experimental import pallas as pl
from jax.experimental.pallas import tpu as pltpu
from jax.sharding import PartitionSpec as P

LEVELS = 4
POINTS = 4
PACK = 16
TURNED = 1
MESH = pl.DeviceIdType.MESH


def to_blocks(source, tile_rows, tile_cols, tile_side):
    channels = source.shape[2]
    shaped = source.reshape(tile_rows, tile_side, tile_cols, tile_side, channels)
    return shaped.transpose(0, 2, 1, 3, 4).reshape(
        tile_rows * tile_cols, tile_side * tile_side, channels
    )


def hat(index, start, low, high):
    return jnp.where(index == start, low, jnp.where(index == start + 1, high, 0.0))


def prepare(head_count, b, query_ref, lw_ref, lb_ref, samples_ref, point_s, corner_s):
    queries_here = query_ref.shape[1]
    hits = LEVELS * POINTS
    logits = lax.dot_general(
        lw_ref[...], query_ref[b], (((1,), (1,)), ((), ())), preferred_element_type=jnp.float32
    ) + lb_ref[...]
    logits = logits.reshape(head_count, hits, queries_here)
    shifted = jnp.exp(logits - jnp.max(logits, axis=1, keepdims=True))
    attend = shifted / jnp.sum(shifted, axis=1, keepdims=True)
    attend = attend.reshape(head_count * hits, queries_here)
    packed = samples_ref[b].T
    pos_row = (packed >> 12) & 4095
    pos_col = packed & 4095
    frac_row = (pos_row & 255).astype(jnp.float32) * (1.0 / 256.0)
    frac_col = (pos_col & 255).astype(jnp.float32) * (1.0 / 256.0)
    point_s[b, 0] = packed >> 24
    point_s[b, 1] = pos_row >> 8
    point_s[b, 2] = pos_col >> 8
    corner_s[b, 0] = attend * (1.0 - frac_row)
    corner_s[b, 1] = attend * frac_row
    corner_s[b, 2] = 1.0 - frac_col
    corner_s[b, 3] = frac_col


def weigh(sides, spans, per_block, b, h, slab, point_s, corner_s, mask_s, weight_s):
    hits = LEVELS * POINTS
    queries_here = weight_s.shape[2]
    lane_row = lax.broadcasted_iota(jnp.int32, (PACK, queries_here), 0)
    slot_row = lax.broadcasted_iota(jnp.int32, (per_block, queries_here), 0)
    level_off = 0
    for level_num in range(LEVELS):
        side = sides[level_num]
        span = spans[level_num]
        rows = [pl.ds(h * hits + level_num * POINTS + p, 1) for p in range(POINTS)]
        for p in range(POINTS):
            mask_s[p * per_block:(p + 1) * per_block, :] = jnp.where(
                slot_row == point_s[b, 0, rows[p], :], 1.0, 0.0
            )
        cols = [
            hat(lane_row % side, point_s[b, 2, rows[p], :], corner_s[b, 2, rows[p], :],
                corner_s[b, 3, rows[p], :])
            for p in range(POINTS)
        ]
        rows_per_chunk = PACK // side

        def chunk(step, carry, rows=rows, cols=cols, side=side, span=span,
                  level_off=level_off, rows_per_chunk=rows_per_chunk):
            parts = []
            for p in range(POINTS):
                index = step * rows_per_chunk
                start = point_s[b, 1, rows[p], :]
                low = corner_s[b, 0, rows[p], :]
                high = corner_s[b, 1, rows[p], :]
                if rows_per_chunk > 1:
                    across = hat(index + lane_row // side, start, low, high)
                else:
                    across = jnp.where(
                        start == index, low, jnp.where(start == index - 1, high, 0.0)
                    )
                parts.append(cols[p] * across)
            for k in range(per_block):
                total = parts[0] * mask_s[k:k + 1, :]
                for p in range(1, POINTS):
                    total = total + parts[p] * mask_s[p * per_block + k:p * per_block + k + 1, :]
                where = pl.multiple_of(level_off + k * span + step * PACK, PACK)
                weight_s[slab, pl.ds(where, PACK), :] = total.astype(jnp.bfloat16)
            return carry

        chunks = span // PACK
        if chunks == 1:
            chunk(0, 0)
        else:
            lax.fori_loop(0, chunks, chunk, 0)
        level_off += span * per_block


def exchange_kernel(sides, spans, per_block, head_count, rows, cols, capacity, local_tiles, *refs):
    (table_ref, tiles_ref, query_ref, lw_ref, lb_ref, samples_ref, fetched_ref, weights_ref) = refs[:8]
    refs = refs[8:]
    held = refs[:cols - 1]
    (ids_v, stage, point_s, corner_s, mask_s, weight_s, id_send, id_recv, col_send, col_recv,
     row_send, row_recv, own_sem, ids_sem, weight_sem) = refs[cols - 1:]
    r = lax.axis_index("row")
    c = lax.axis_index("col")
    lanes_wide = tiles_ref.shape[1]
    barrier = pltpu.get_barrier_semaphore()
    for dc in range(1, cols):
        pl.semaphore_signal(barrier, inc=1, device_id={"col": lax.rem(c + dc, cols)}, device_id_type=MESH)
    for dr in range(1, rows):
        pl.semaphore_signal(barrier, inc=1, device_id={"row": lax.rem(r + dr, rows)}, device_id_type=MESH)
    pl.semaphore_wait(barrier, cols + rows - 2)

    id_copies = []
    for dr in range(1, rows):
        to = lax.rem(r + dr, rows)
        copy = pltpu.make_async_remote_copy(
            table_ref.at[to], ids_v.at[dr], id_send.at[dr], id_recv.at[dr],
            device_id={"row": to}, device_id_type=MESH,
        )
        copy.start()
        id_copies.append(copy)
    col_copies = []
    for dc in range(1, cols):
        copy = pltpu.make_async_remote_copy(
            tiles_ref, held[dc - 1], col_send.at[dc], col_recv.at[dc],
            device_id={"col": lax.rem(c + dc, cols)}, device_id_type=MESH,
        )
        copy.start()
        col_copies.append(copy)
    own_ids = pltpu.make_async_copy(table_ref.at[r], ids_v.at[0], ids_sem)
    own_ids.start()
    own_ids.wait()
    for copy in id_copies:
        copy.wait()

    def pick(dc):
        owner_col = lax.rem(c - dc + cols, cols)
        source = tiles_ref if dc == 0 else held[dc - 1]
        out_at = (r * cols + owner_col) * capacity
        copies = []
        for turn in range(rows):
            dr = (turn + 1) % rows
            for place in range(capacity):
                off = 0
                for level_num in range(LEVELS):
                    span = spans[level_num]
                    at = (owner_col * capacity + place) * LEVELS + level_num
                    asked = jnp.broadcast_to(ids_v[dr, pl.ds(at, 1), :], (PACK, lanes_wide))
                    shape = (span // PACK, PACK, lanes_wide)
                    total = None
                    for tile in range(local_tiles):
                        mask = jnp.where(asked == tile, 1.0, 0.0).astype(jnp.bfloat16)
                        first = local_tiles * off + tile * span
                        part = source[first:first + span, :].reshape(shape) * mask[None]
                        total = part if total is None else total + part
                    stage[dr, dc, place, off:off + span, :] = total.reshape(span, lanes_wide)
                    off += span
            target = fetched_ref.at[pl.ds(out_at, capacity)]
            if dr == 0:
                copy = pltpu.make_async_copy(stage.at[dr, dc], target, own_sem.at[dc])
            else:
                copy = pltpu.make_async_remote_copy(
                    stage.at[dr, dc], target, row_send.at[dr, dc], row_recv.at[dr, dc],
                    device_id={"row": lax.rem(r - dr + rows, rows)}, device_id_type=MESH,
                )
            copy.start()
            copies.append(copy)
        return copies

    copies = pick(0)

    def prepare_one(b, carry):
        prepare(head_count, b, query_ref, lw_ref, lb_ref, samples_ref, point_s, corner_s)
        return carry

    lax.fori_loop(0, local_tiles, prepare_one, 0)

    def store(step, slab):
        return pltpu.make_async_copy(
            weight_s.at[slab], weights_ref.at[step // head_count, step % head_count],
            weight_sem.at[slab],
        )

    def weigh_one(step, carry):
        slab = step % 2

        @pl.when(step >= 2)
        def _():
            store(step - 2, slab).wait()

        weigh(sides, spans, per_block, step // head_count, step % head_count, slab,
              point_s, corner_s, mask_s, weight_s)
        store(step, slab).start()
        return carry

    steps = local_tiles * head_count
    done = 0
    for dc in range(1, cols):
        until = steps * dc // (cols - 1)
        if until > done:
            lax.fori_loop(done, until, weigh_one, 0)
        done = until
        col_copies[dc - 1].wait()
        copies += pick(dc)
    for step in range(max(0, steps - 2), steps):
        store(step, step % 2).wait()
    for copy in copies:
        copy.wait()


def mix_kernel(spans, per_block, head_count, head_dim, pos_ref, fetched_ref, upper_ref, lower_ref,
               out_ref,
               values, values_t, mixed, sem):
    block = pl.program_id(0)
    h = pl.program_id(1)
    blocks = pl.num_programs(0)

    def fetch(which):
        off = 0
        src = 0
        for level_num in range(LEVELS):
            span = spans[level_num]
            for k in range(per_block):
                pltpu.make_async_copy(
                    fetched_ref.at[pos_ref[level_num, which * per_block + k], pl.ds(src, span), :],
                    values.at[which % 2, pl.ds(off, span), :],
                    sem.at[which % 2],
                ).start()
                off += span
            src += span

    @pl.when((h == 0) & (block == 0))
    def _():
        fetch(block)

    @pl.when(h == 0)
    def _():
        side = block % 2
        pltpu.make_async_copy(values.at[side], values.at[side], sem.at[side]).wait()
        values_t[...] = values[side].T.reshape(values_t.shape)

        @pl.when(block + 1 < blocks)
        def _():
            fetch(block + 1)

    half = upper_ref.shape[2]
    mixed[h] = jnp.dot(
        values_t[h, :, :half], upper_ref[0, 0], preferred_element_type=jnp.float32
    ) + jnp.dot(values_t[h, :, half:], lower_ref[0, 0], preferred_element_type=jnp.float32)

    @pl.when(h == head_count - 1)
    def _():
        whole = mixed[...].reshape(head_count * head_dim, mixed.shape[2])
        out_ref[...] = whole.T.astype(jnp.bfloat16)


def gathered_attention(queries, level_blocks, tile_lists, samples, logit_weight, logit_bias, sides, spans):
    row_count = lax.axis_size("row")
    col_count = lax.axis_size("col")
    peer_count = row_count * col_count
    tile_rows, tile_cols, level_count, per_block = tile_lists.shape
    local_tiles = tile_rows * tile_cols
    requests = local_tiles * per_block
    capacity = max(2, (requests + peer_count - 1) // peer_count)
    slots = peer_count * capacity
    grid_cols = tile_cols * col_count
    channels = level_blocks[0].shape[2]
    head_count = samples.shape[2] // (LEVELS * POINTS)
    head_dim = channels // head_count
    tile_side = sides[0]
    pixels = tile_side * tile_side
    tile_span = sum(spans)
    depth = per_block * tile_span

    wanted = tile_lists.transpose(2, 0, 1, 3).reshape(level_count, requests)
    grid_row = wanted // grid_cols
    grid_col = wanted % grid_cols
    owner_dev = grid_row // tile_rows * col_count + grid_col // tile_cols
    local_index = grid_row % tile_rows * tile_cols + grid_col % tile_cols
    order = jnp.arange(requests, dtype=jnp.int32)
    earlier = (owner_dev[:, :, None] == owner_dev[:, None, :]) & (order[None, :] < order[:, None])
    positions = owner_dev * capacity + jnp.sum(earlier.astype(jnp.int32), axis=2)
    slot_order = jnp.arange(slots, dtype=jnp.int32)
    named = positions[:, None, :] == slot_order[None, :, None]
    slot_table = jnp.max(jnp.where(named, local_index[:, None, :], -1), axis=2)
    table = jnp.maximum(slot_table, 0).reshape(level_count, row_count, col_count * capacity)
    table = table.transpose(1, 2, 0).reshape(row_count, col_count * capacity * level_count, 1)
    table_rows = table.shape[1]
    table = jnp.broadcast_to(table, (row_count, table_rows, channels))

    tiles_local = []
    for level_num in range(level_count):
        tiles = to_blocks(level_blocks[level_num], tile_rows, tile_cols, sides[level_num])
        short = spans[level_num] - tiles.shape[1]
        if short > 0:
            tiles = jnp.pad(tiles, ((0, 0), (0, short), (0, 0)))
        tiles_local.append(tiles.reshape(local_tiles * spans[level_num], channels))
    tiles_local = jnp.concatenate(tiles_local, axis=0)

    queries_blocked = to_blocks(queries, tile_rows, tile_cols, tile_side)
    samples_blocked = to_blocks(samples, tile_rows, tile_cols, tile_side)
    lanes = head_count * LEVELS * POINTS
    vmem = pl.BlockSpec(memory_space=pltpu.VMEM)
    whole = pl.BlockSpec(memory_space=pl.ANY)
    dma = pltpu.SemaphoreType.DMA
    fetched, weights = pl.pallas_call(
        functools.partial(exchange_kernel, sides, spans, per_block, head_count, row_count,
                          col_count, capacity, local_tiles),
        out_shape=(
            jax.ShapeDtypeStruct((slots, tile_span, channels), jnp.bfloat16),
            jax.ShapeDtypeStruct((local_tiles, head_count, depth, pixels), jnp.bfloat16),
        ),
        in_specs=[vmem] * 6,
        out_specs=(whole, whole),
        scratch_shapes=[
            pltpu.VMEM((local_tiles * tile_span, channels), jnp.bfloat16)
            for _ in range(col_count - 1)
        ] + [
            pltpu.VMEM((row_count, table_rows, channels), jnp.int32),
            pltpu.VMEM((row_count, col_count, capacity, tile_span, channels), jnp.bfloat16),
            pltpu.VMEM((local_tiles, 3, lanes, pixels), jnp.int32),
            pltpu.VMEM((local_tiles, 4, lanes, pixels), jnp.float32),
            pltpu.VMEM((POINTS * per_block, pixels), jnp.float32),
            pltpu.VMEM((2, depth, pixels), jnp.bfloat16),
            dma((row_count,)), dma((row_count,)), dma((col_count,)), dma((col_count,)),
            dma((row_count, col_count)), dma((row_count, col_count)), dma((col_count,)),
            dma, dma((2,)),
        ],
        compiler_params=pltpu.CompilerParams(
            collective_id=0, has_side_effects=True, vmem_limit_bytes=60 * 1024 * 1024
        ),
        cost_estimate=pl.CostEstimate(
            flops=8 * local_tiles * head_count * depth * pixels * POINTS,
            bytes_accessed=2 * local_tiles * head_count * depth * pixels, transcendentals=0,
        ),
        name="exchange",
    )(table, tiles_local, queries_blocked, logit_weight.T, logit_bias[:, None], samples_blocked)

    attn_out = pl.pallas_call(
        functools.partial(mix_kernel, spans, per_block, head_count, head_dim),
        grid_spec=pltpu.PrefetchScalarGridSpec(
            num_scalar_prefetch=1,
            grid=(local_tiles, head_count),
            in_specs=[
                pl.BlockSpec(memory_space=pl.ANY),
                pl.BlockSpec((1, 1, depth // 2, pixels), lambda b, h, pos: (b, h, 0, 0)),
                pl.BlockSpec((1, 1, depth // 2, pixels), lambda b, h, pos: (b, h, 1, 0)),
            ],
            out_specs=pl.BlockSpec((pixels, channels), lambda b, h, pos: (b, 0)),
            scratch_shapes=[
                pltpu.VMEM((2, depth, channels), jnp.bfloat16),
                pltpu.VMEM((head_count, head_dim, depth), jnp.bfloat16),
                pltpu.VMEM((head_count, head_dim, pixels), jnp.float32),
                pltpu.SemaphoreType.DMA((2,)),
            ],
        ),
        out_shape=jax.ShapeDtypeStruct((local_tiles * pixels, channels), jnp.bfloat16),
        compiler_params=pltpu.CompilerParams(
            dimension_semantics=("arbitrary", "arbitrary"), vmem_limit_bytes=60 * 1024 * 1024
        ),
        cost_estimate=pl.CostEstimate(
            flops=2 * local_tiles * depth * pixels * channels,
            bytes_accessed=2 * local_tiles * head_count * depth * pixels, transcendentals=0,
        ),
        name="mix",
    )(positions, fetched, weights, weights)
    return attn_out


def power_of_two(n):
    return n > 0 and n & (n - 1) == 0


def group_order(c, cols):
    near = jnp.minimum(c, cols - 1 - c)
    order = [c]
    for g in range(1, cols):
        both = c - (g + 1) // 2 if g % 2 else c + g // 2
        one = jnp.where(c < cols - 1 - c, c + g - near, c - g + near)
        order.append(jnp.where(g <= 2 * near, both, one))
    return order


def plan_tables(rows, cols, per_block, lists_ref, table, turned_table, index_v):
    blocks = lists_ref.shape[0]
    wanted = jnp.concatenate([lists_ref[b] for b in range(blocks)], axis=1)
    requests = wanted.shape[1]
    tile_rows = blocks
    col_bits = cols.bit_length() - 1
    row_bits = tile_rows.bit_length() - 1
    shape = (requests, requests)
    down = lax.broadcasted_iota(jnp.int32, shape, 0)
    along = lax.broadcasted_iota(jnp.int32, shape, 1)
    capacity = requests // (rows * cols)
    for level_num in range(LEVELS):
        here = jnp.broadcast_to(wanted[level_num:level_num + 1, :], shape)
        if level_num == TURNED:
            own_here = (here & (cols - 1)) * rows + (here >> (col_bits + row_bits))
        else:
            own_here = ((here >> (col_bits + row_bits)) << col_bits) + (here & (cols - 1))
        local_here = (here >> col_bits) & (tile_rows - 1)
        same = own_here == own_here.T
        place_here = jnp.sum(jnp.where(same & (down < along), 1, 0), axis=0, keepdims=True)
        slot_here = own_here * capacity + place_here
        asked = jnp.sum(
            jnp.where(slot_here == down, local_here.astype(jnp.float32), 0.0), axis=1, keepdims=True
        )
        asked = jnp.broadcast_to(asked, (requests, table.shape[3])).astype(jnp.int32)
        if level_num == TURNED:
            turned_table[...] = asked.reshape(turned_table.shape)
        else:
            table[:, level_num] = asked.reshape(rows, requests // rows, table.shape[3])
        filled = jnp.sum(jnp.where(slot_here.T == along, down, 0), axis=0, keepdims=True)
        index_v[level_num:level_num + 1, 0:requests] = filled


def points(head_count, b, query_ref, lw_ref, bias, samples_ref, point_s, corner_s, slot_s):
    queries_here = query_ref.shape[1]
    hits = LEVELS * POINTS
    logits = lax.dot_general(
        lw_ref[...], query_ref[b], (((1,), (1,)), ((), ())), preferred_element_type=jnp.float32
    ) + bias
    logits = logits.reshape(head_count, hits, queries_here)
    shifted = jnp.exp(logits - jnp.max(logits, axis=1, keepdims=True))
    attend = shifted / jnp.sum(shifted, axis=1, keepdims=True)
    attend = attend.reshape(head_count * hits, queries_here)
    packed = samples_ref[b].T
    pos_row = (packed >> 12) & 4095
    pos_col = packed & 4095
    frac_row = (pos_row & 255).astype(jnp.float32) * (1.0 / 256.0)
    frac_col = (pos_col & 255).astype(jnp.float32) * (1.0 / 256.0)
    point_s[b, 0] = pos_row >> 8
    point_s[b, 1] = pos_col >> 8
    corner_s[b, 0] = attend * (1.0 - frac_row)
    corner_s[b, 1] = attend * frac_row
    corner_s[b, 2] = 1.0 - frac_col
    corner_s[b, 3] = frac_col
    slot_s[b] = (packed >> 24).astype(jnp.float32)


def hats(start, low, high, count):
    here = [start == i for i in range(count)]
    out = [jnp.where(here[0], low, 0.0)]
    for i in range(1, count):
        out.append(jnp.where(here[i], low, jnp.where(here[i - 1], high, 0.0)))
    return out


def weigh_block(sides, spans, per_block, head_count, step, point_s, corner_s, slot_s, down_s, spread_s,
                weight_s):
    hits = LEVELS * POINTS
    queries_here = spread_s.shape[2]
    b = step // head_count
    h = step % head_count
    half = PACK // 2
    lane_row = lax.broadcasted_iota(jnp.int32, (PACK, queries_here), 0)
    off = 0
    for level_num in range(LEVELS):
        side = sides[level_num]
        span = spans[level_num]
        for p in range(POINTS):
            row = pl.ds(h * hits + level_num * POINTS + p, 1)
            across = hat(lane_row % side, point_s[b, 1, row, :], corner_s[b, 2, row, :],
                         corner_s[b, 3, row, :])
            down = hat(lane_row // side if side < half else lane_row, point_s[b, 0, row, :],
                       corner_s[b, 0, row, :], corner_s[b, 1, row, :])
            if side >= half:
                at_down = (level_num * POINTS + p) * PACK
                down_s[at_down:at_down + PACK, :] = down
                for chunk in range(span // PACK):
                    parts = []
                    for part in range(2):
                        at = chunk * PACK + part * half
                        col = at % side if side > half else part * half
                        line = at_down + at // side
                        parts.append(across[col:col + half, :] * down_s[line:line + 1, :])
                    total = jnp.concatenate(parts, axis=0).astype(jnp.bfloat16)
                    spread_s[p, off + chunk * PACK:off + (chunk + 1) * PACK, :] = total
            else:
                spread_s[p, off:off + PACK, :] = (across * down).astype(jnp.bfloat16)
        off += span
    off = 0
    quad = 4
    one = jnp.ones((PACK, queries_here), jnp.bfloat16)
    none = jnp.zeros((PACK, queries_here), jnp.bfloat16)
    for level_num in range(LEVELS):
        span = spans[level_num]
        slots = []
        for p in range(POINTS):
            mine = slot_s[b, pl.ds(h * hits + level_num * POINTS + p, 1), :]
            slots.append(jnp.broadcast_to(mine, (PACK, queries_here)).astype(jnp.bfloat16))
        for first in range(0, per_block, quad):
            masks = []
            for k in range(first, first + quad):
                label = jnp.full((PACK, queries_here), k, jnp.bfloat16)
                masks.append([jnp.where(slots[p] == label, one, none) for p in range(POINTS)])
            for chunk in range(span // PACK):
                pieces = [spread_s[p, off + chunk * PACK:off + (chunk + 1) * PACK, :] for p in range(POINTS)]
                for k in range(first, first + quad):
                    total = pieces[0] * masks[k - first][0]
                    for p in range(1, POINTS):
                        total = total + pieces[p] * masks[k - first][p]
                    weight_s[level_num][step * per_block + k, chunk * PACK:(chunk + 1) * PACK, :] = total
        off += span


def mix_slots(spans, per_block, head_count, head_dim, rows, cols, blocks, pieces, index_s, fetched,
              turned, keep_s, weight_s, mixed, finish):
    capacity = 2
    units = rows * capacity
    lanes = 128
    block_bits = per_block.bit_length() - 1
    requests = blocks * per_block
    lane = lax.broadcasted_iota(jnp.int32, (1, lanes), 1)

    def entry_of(group, level_num, unit):
        if level_num == TURNED:
            slot = group * units + unit
        else:
            slot = (unit // capacity * cols + group) * capacity + unit % capacity
        return index_s[level_num, slot] & (requests - 1)

    owners = []
    depth = 0
    for group, level_num in pieces:
        span = spans[level_num]
        size = units * span
        at = units * sum(spans[:level_num])
        turned[:, depth:depth + size] = fetched[group, at:at + size, :].T
        depth += size
        block_of = [entry_of(group, level_num, unit) >> block_bits for unit in range(units)]
        for start in range(0, size, lanes):
            first = start // span
            last = (start + lanes - 1) // span
            value = jnp.full((1, lanes), block_of[first], jnp.int32)
            for unit in range(first + 1, last + 1):
                value = jnp.where(lane >= unit * span - start, block_of[unit], value)
            owners.append(value)
    owner_row = jnp.concatenate(owners, axis=1)
    for b in range(blocks):
        keep_s[b, :, 0:depth] = jnp.broadcast_to(
            jnp.where(owner_row == b, 1.0, 0.0), (PACK, depth)
        ).astype(jnp.bfloat16)

    def one_head(h, carry):
        left = jnp.concatenate([
            turned[pl.ds(pl.multiple_of(h * head_dim + half, PACK), PACK), 0:depth]
            * keep_s[b, :, 0:depth]
            for b in range(blocks) for half in range(0, head_dim, PACK)
        ], axis=0)
        right = []
        for group, level_num in pieces:
            for unit in range(units):
                entry = entry_of(group, level_num, unit)
                source = (entry >> block_bits) * head_count + h
                right.append(weight_s[level_num][source * per_block + (entry & (per_block - 1))])
        right = jnp.concatenate(right, axis=0)
        total = mixed[h] + jnp.dot(left, right, preferred_element_type=jnp.float32)
        finish(h, total)
        return carry

    lax.fori_loop(0, head_count, one_head, 0)


def fused_kernel(sides, spans, per_block, head_count, head_dim, rows, cols, *refs):
    sources, refs = refs[:13], refs[13:]
    out_ref, refs = refs[0], refs[1:]
    held, refs = refs[:10], refs[10:]
    (lists_ref, three_ref, query_ref, lw_ref, lb_ref, samples_ref, ow_ref, ob_ref,
     gain_ref, shift_ref) = held
    (layer_v, turned_table, turned_ids, turned_stage, blocks_v, table, ids_v, stage, fetched, index_v, index_s, point_s,
     corner_s, slot_s, down_s, spread_s, weight_0, weight_1, weight_2, weight_3, turned, keep_s, mixed,
     attn_own, attn_other, id_send, id_recv, up_send, up_recv, down_send, down_recv, row_send, row_recv,
     head_send, head_recv, layer_send, layer_recv, list_send, list_recv, turned_send, turned_recv,
     index_sem, in_sem) = refs
    weight_s = (weight_0, weight_1, weight_2, weight_3)
    local_tiles = lists_ref.shape[0]
    capacity = 2
    r = lax.axis_index("row")
    c = lax.axis_index("col")
    head = lax.axis_index("head")
    lanes_wide = blocks_v.shape[2]
    starts = {}
    off = 0
    for level_num in range(LEVELS):
        if level_num != TURNED:
            starts[level_num] = off
            off += local_tiles * (spans[level_num] if level_num < LEVELS - 1 else PACK // 2)
    targets = [
        layer_v.at[r] if level_num == TURNED
        else blocks_v.at[c, pl.ds(starts[level_num], local_tiles * spans[level_num])]
        for level_num in range(3)
    ]
    loads = [
        pltpu.make_async_copy(source, target, in_sem.at[i])
        for i, (source, target) in enumerate(zip(sources, targets + list(held)))
    ]
    for load in loads:
        load.start()
    barrier = pltpu.get_barrier_semaphore()
    pl.semaphore_signal(barrier, inc=1, device_id={"head": 1 - head}, device_id_type=MESH)
    for dr in range(1, rows):
        pl.semaphore_signal(barrier, inc=1, device_id={"row": lax.rem(r + dr, rows)}, device_id_type=MESH)
    for dc in range(1, cols):
        pl.semaphore_signal(barrier, inc=1, device_id={"col": lax.rem(c + dc, cols)}, device_id_type=MESH)
    for load in loads[3:5]:
        load.wait()
    span = PACK // 2
    side = sides[3]
    for tile in range(local_tiles):
        rows_here = jnp.concatenate(
            [three_ref[tile * side + i].astype(jnp.float32) for i in range(side)]
            + [jnp.zeros((span - side * side, lanes_wide), jnp.float32)], axis=0
        )
        at = starts[3] + tile * span
        blocks_v[c, at:at + span, :] = rows_here.astype(jnp.bfloat16)
    depth = fetched.shape[1]
    padded = rows * capacity * spans[3]
    fetched[:, depth - padded:depth, :] = jnp.zeros((cols, padded, lanes_wide), jnp.bfloat16)
    plan_tables(rows, cols, per_block, lists_ref, table, turned_table, index_v)

    for load in loads[:3]:
        load.wait()
    pl.semaphore_wait(barrier, rows + cols - 1)

    block_rows = blocks_v.shape[1]
    parts = 2
    part_rows = block_rows // parts

    def up(block, part):
        at = blocks_v.at[block, pl.ds(pl.multiple_of(part * part_rows, PACK), part_rows)]
        return pltpu.make_async_remote_copy(
            at, at, up_send.at[c - block, part], up_recv.at[c - block, part],
            device_id={"col": c + 1}, device_id_type=MESH,
        )

    def down(block, part):
        at = blocks_v.at[block, pl.ds(pl.multiple_of(part * part_rows, PACK), part_rows)]
        return pltpu.make_async_remote_copy(
            at, at, down_send.at[block - c, part], down_recv.at[block - c, part],
            device_id={"col": c - 1}, device_id_type=MESH,
        )

    def came_up(block, part):
        at = blocks_v.at[block, pl.ds(pl.multiple_of(part * part_rows, PACK), part_rows)]
        return pltpu.make_async_remote_copy(
            at, at, up_send.at[c - 1 - block, part], up_recv.at[c - 1 - block, part],
            device_id={"col": c - 1}, device_id_type=MESH,
        )

    def came_down(block, part):
        at = blocks_v.at[block, pl.ds(pl.multiple_of(part * part_rows, PACK), part_rows)]
        return pltpu.make_async_remote_copy(
            at, at, down_send.at[block - c - 1, part], down_recv.at[block - c - 1, part],
            device_id={"col": c + 1}, device_id_type=MESH,
        )

    def id_copy(dr):
        to = lax.rem(r + dr, rows)
        return pltpu.make_async_remote_copy(
            table.at[to], ids_v.at[dr], id_send.at[dr], id_recv.at[dr],
            device_id={"row": to}, device_id_type=MESH,
        )

    def list_copy(dc):
        to = lax.rem(c + dc, cols)
        return pltpu.make_async_remote_copy(
            turned_table.at[to], turned_ids.at[c], list_send.at[dc], list_recv.at[dc],
            device_id={"col": to}, device_id_type=MESH,
        )

    def layer_copy(dr):
        return pltpu.make_async_remote_copy(
            layer_v.at[r], layer_v.at[r], layer_send.at[dr], layer_recv.at[dr],
            device_id={"row": lax.rem(r + dr, rows)}, device_id_type=MESH,
        )

    def layer_came(dr):
        at = layer_v.at[lax.rem(r - dr + rows, rows)]
        return pltpu.make_async_remote_copy(
            at, at, layer_send.at[dr], layer_recv.at[dr],
            device_id={"row": lax.rem(r + dr, rows)}, device_id_type=MESH,
        )

    def list_came(dc):
        return pltpu.make_async_remote_copy(
            turned_table.at[c], turned_ids.at[lax.rem(c - dc + cols, cols)], list_send.at[dc],
            list_recv.at[dc], device_id={"col": lax.rem(c + dc, cols)}, device_id_type=MESH,
        )

    for dr in range(1, rows):
        id_copy(dr).start()
    for dc in range(1, cols):
        list_copy(dc).start()
    for part in range(parts):
        @pl.when(c < cols - 1)
        def _(part=part):
            up(c, part).start()

        @pl.when(c > 0)
        def _(part=part):
            down(c, part).start()

    for dr in range(1, rows):
        layer_copy(dr).start()
    turned_ids[c] = turned_table[c]
    ids_v[0] = table[r]
    for load in loads[5:]:
        load.wait()
    bias = jnp.broadcast_to(lb_ref[...], (8, lb_ref.shape[1])).T[:, 0:1]

    def points_one(b, carry):
        points(head_count, b, query_ref, lw_ref, bias, samples_ref, point_s, corner_s, slot_s)
        return carry

    lax.fori_loop(0, local_tiles, points_one, 0)
    index_copy = pltpu.make_async_copy(index_v, index_s, index_sem)
    index_copy.start()
    def relay(step, part):
        @pl.when(c - 1 - step >= 0)
        def _():
            block = c - 1 - step
            came_up(block, part).wait_recv()

            @pl.when(c < cols - 1)
            def _():
                up(block, part).start()

        @pl.when(c + 1 + step < cols)
        def _():
            block = c + 1 + step
            came_down(block, part).wait_recv()

            @pl.when(c > 0)
            def _():
                down(block, part).start()

    half = PACK // 2
    last = LEVELS - 1

    def row_copy(block, dr, level_num):
        kind = last if level_num == TURNED else level_num
        span = spans[kind]
        first = capacity * sum(spans[:kind])
        size = capacity * span
        to = rows * first + r * size
        if kind == last:
            place = 1 if level_num == TURNED else 0
            first, to, size = first + place * span, to + place * span, half
        return pltpu.make_async_remote_copy(
            stage.at[block, dr - 1, pl.ds(first, size)],
            fetched.at[block, pl.ds(pl.multiple_of(to, half), size)],
            row_send.at[block, dr, level_num], row_recv.at[block, dr, level_num],
            device_id={"row": lax.rem(r - dr + rows, rows)}, device_id_type=MESH,
        )

    across = sorted(range(1, rows), key=lambda dr: dr != rows // 2) + [0]

    def pick(block, first_use=False):
        for dr in across:
            if first_use and dr != 0:
                id_copy(dr).wait()
            off = 0
            for level_num in range(LEVELS):
                span = spans[level_num]
                size = capacity * span
                if level_num == TURNED:
                    off += span
                    continue
                held_rows = half if level_num == last else span
                pack = min(PACK, held_rows)
                for place in range(capacity):
                    asked = jnp.broadcast_to(
                        ids_v[dr, level_num, pl.ds(block * capacity + place, 1), :], (pack, lanes_wide)
                    )
                    total = None
                    for tile in range(local_tiles):
                        mask = jnp.where(asked == tile, 1.0, 0.0).astype(jnp.bfloat16)
                        first = starts[level_num] + tile * held_rows
                        part = blocks_v[block, first:first + held_rows, :].reshape(
                            held_rows // pack, pack, lanes_wide) * mask[None]
                        total = part if total is None else total + part
                    total = total.reshape(held_rows, lanes_wide)
                    if dr == 0:
                        at = pl.multiple_of(rows * capacity * off + r * size + place * span, span)
                        fetched[block, pl.ds(at, held_rows), :] = total
                    else:
                        at = capacity * off + place * span
                        stage[block, dr - 1, at:at + held_rows, :] = total
                if dr != 0:
                    row_copy(block, dr, level_num).start()
                    if level_num == last:
                        row_copy(block, dr, TURNED).start()
                off += span

    turned_span = spans[TURNED]
    turned_at = rows * capacity * sum(spans[:TURNED])
    turned_size = rows * capacity * turned_span

    def turned_copy(block, to):
        return pltpu.make_async_remote_copy(
            turned_stage.at[to], fetched.at[block, pl.ds(turned_at, turned_size)],
            turned_send.at[to], turned_recv.at[block],
            device_id={"col": to}, device_id_type=MESH,
        )

    def pick_turned(to, target, base):
        for owner in range(rows):
            for place in range(capacity):
                unit = owner * capacity + place
                asked = jnp.broadcast_to(turned_ids[to, pl.ds(unit, 1), :], (PACK, lanes_wide))
                total = None
                for tile in range(local_tiles):
                    mask = jnp.where(asked == tile, 1.0, 0.0).astype(jnp.bfloat16)
                    part = layer_v[owner, tile * turned_span:(tile + 1) * turned_span, :].reshape(
                        turned_span // PACK, PACK, lanes_wide) * mask[None]
                    total = part if total is None else total + part
                at = base + unit * turned_span
                target[at:at + turned_span, :] = total.reshape(turned_span, lanes_wide)

    def send_turned(step):
        for to, before in ((step + 1, True), (cols - 2 - step, False)):
            @pl.when(c < to if before else c > to)
            def _(to=to):
                pick_turned(to, turned_stage.at[to], 0)
                turned_copy(c, to).start()

    def settle(block):
        for dr in range(1, rows):
            for level_num in range(LEVELS):
                row_copy(block, dr, level_num).wait_recv()

    def weigh(first, last):
        def one(step, carry):
            weigh_block(sides, spans, per_block, head_count, step, point_s, corner_s, slot_s, down_s,
                        spread_s, weight_s)
            return carry

        lax.fori_loop(first, last, one, 0)

    def head_copy(h):
        return pltpu.make_async_remote_copy(
            attn_own.at[h], attn_other.at[h], head_send.at[h], head_recv.at[h],
            device_id={"head": 1 - head}, device_id_type=MESH,
        )

    def keep_sum(h, total):
        mixed[h] = total

    def send_sum(h, total):
        attn_own[h] = total.astype(jnp.bfloat16)
        head_copy(h).start()

    straight = [level_num for level_num in range(LEVELS) if level_num != TURNED]

    def mix(pieces, finish=keep_sum):
        mix_slots(spans, per_block, head_count, head_dim, rows, cols, local_tiles, pieces, index_s,
                  fetched, turned, keep_s, weight_s, mixed, finish)

    def mix_straight(block, finish=keep_sum):
        settle(block)
        mix([(block, level_num) for level_num in straight], finish)

    order = group_order(c, cols)
    mixed[...] = jnp.zeros_like(mixed)
    pick(order[0], True)
    total_steps = local_tiles * head_count
    index_copy.wait()

    def relay_and_weigh(step, share):
        def one(part, carry):
            first = (step * parts + part) * share
            weigh(jnp.minimum(first, total_steps), jnp.minimum(first + share, total_steps))
            relay(step, part)
            return carry

        lax.fori_loop(0, parts, one, 0)

    for g in range(1, cols):
        relay_and_weigh(g - 1, -(-total_steps // (parts * (cols - 1))))
        pick(order[g])
        if g == 1:
            for dr in range(1, rows):
                layer_came(dr).wait_recv()
            for dc in range(1, cols):
                list_came(dc).wait_recv()
            pick_turned(c, fetched.at[c], turned_at)
        send_turned(g - 1)
    settle(order[0])
    mix([(order[0], level_num) for level_num in range(LEVELS)])
    for g in range(1, cols - 1):
        mix_straight(order[g])
    for g in range(1, cols):
        turned_copy(order[g], order[g]).wait_recv()
    mix([(order[g], TURNED) for g in range(1, cols)])

    def row_sent(block):
        for dr in range(1, rows):
            for level_num in range(LEVELS):
                row_copy(block, dr, level_num).wait_send()

    for dr in range(1, rows):
        layer_copy(dr).wait_send()
    for dc in range(1, cols):
        list_copy(dc).wait_send()
        turned_copy(c, lax.rem(c + dc, cols)).wait_send()
    for g in range(cols - 1):
        row_sent(order[g])
    for block in range(cols):
        for part in range(parts):
            @pl.when((block <= c) & (c < cols - 1))
            def _(block=block, part=part):
                up(block, part).wait_send()

            @pl.when((block >= c) & (c > 0))
            def _(block=block, part=part):
                down(block, part).wait_send()

    mix_straight(order[cols - 1], send_sum)
    row_sent(order[cols - 1])

    size = mixed.shape[2]
    ch = head_count * head_dim
    own_at = pl.multiple_of(head * ch, ch)
    other_at = pl.multiple_of((1 - head) * ch, ch)
    for h in range(head_count):
        head_copy(h).wait()

    def finish_block(b, carry):
        here = pl.ds(pl.multiple_of(b * head_dim, head_dim), head_dim)
        own = jnp.concatenate([attn_own[h, here, :] for h in range(head_count)], axis=0)
        other = jnp.concatenate([attn_other[h, here, :] for h in range(head_count)], axis=0)

        def project(at):
            lanes = pl.ds(at, ch)
            add = lax.dot_general(
                own, ow_ref[pl.ds(own_at, ch), lanes], (((0,), (0,)), ((), ())),
                preferred_element_type=jnp.float32,
            ) + lax.dot_general(
                other, ow_ref[pl.ds(other_at, ch), lanes], (((0,), (0,)), ((), ())),
                preferred_element_type=jnp.float32,
            )
            return query_ref[b, :, lanes].astype(jnp.float32) + add + ob_ref[:, lanes]

        mine = project(own_at)
        rest = project(other_at)
        scale = 1.0 / (2 * ch)
        mean = jnp.sum(mine + rest, axis=1, keepdims=True) * scale
        mine = mine - mean
        rest = rest - mean
        variance = jnp.sum(mine * mine + rest * rest, axis=1, keepdims=True) * scale
        normed = mine * lax.rsqrt(variance + 1e-05) * gain_ref[...] + shift_ref[...]
        out_ref[pl.ds(pl.multiple_of(b * size, size), size), :] = normed.astype(jnp.bfloat16)
        return carry

    lax.fori_loop(0, local_tiles, finish_block, 0)


def fused_layer(queries, level_blocks, tile_lists, samples, logit_weight, logit_bias, output_weight,
                output_bias, norm_gain, norm_shift, sides, spans):
    rows = lax.axis_size("row")
    cols = lax.axis_size("col")
    tile_rows, tile_cols, level_count, per_block = tile_lists.shape
    local_tiles = tile_rows * tile_cols
    requests = local_tiles * per_block
    channels = level_blocks[0].shape[2]
    lanes = samples.shape[2]
    head_count = lanes // (LEVELS * POINTS)
    head_dim = channels // head_count
    pixels = spans[0]
    tile_span = sum(spans)
    capacity = requests // (rows * cols)
    depth = rows * capacity * tile_span
    flat = [level.reshape(-1, channels) for level in level_blocks[:3]]
    held = (
        tile_lists.reshape(local_tiles, level_count, per_block), level_blocks[3],
        queries.reshape(local_tiles, pixels, queries.shape[2]), logit_weight.T, logit_bias[None, :],
        samples.reshape(local_tiles, pixels, lanes), output_weight, output_bias[None, :],
        norm_gain[None, :], norm_shift[None, :],
    )
    vmem = pl.BlockSpec(memory_space=pltpu.VMEM)
    dma = pltpu.SemaphoreType.DMA
    parts = 2
    return pl.pallas_call(
        functools.partial(fused_kernel, sides, spans, per_block, head_count, head_dim, rows, cols),
        out_shape=jax.ShapeDtypeStruct((local_tiles * pixels, channels), jnp.bfloat16),
        in_specs=[pl.BlockSpec(memory_space=pltpu.HBM)] * 13,
        out_specs=vmem,
        scratch_shapes=[
            *[pltpu.VMEM(one.shape, one.dtype) for one in held],
            pltpu.VMEM((rows, local_tiles * spans[TURNED], channels), jnp.bfloat16),
            pltpu.VMEM((cols, requests // cols, channels), jnp.int32),
            pltpu.VMEM((cols, requests // cols, channels), jnp.int32),
            pltpu.VMEM((cols, rows * capacity * spans[TURNED], channels), jnp.bfloat16),
            pltpu.VMEM((cols, local_tiles * (tile_span - spans[TURNED] - PACK // 2), channels), jnp.bfloat16),
            pltpu.VMEM((rows, LEVELS, requests // rows, channels), jnp.int32),
            pltpu.VMEM((rows, LEVELS, requests // rows, channels), jnp.int32),
            pltpu.VMEM((cols, rows - 1, capacity * tile_span, channels), jnp.bfloat16),
            pltpu.VMEM((cols, depth, channels), jnp.bfloat16),
            pltpu.VMEM((8, 128), jnp.int32),
            pltpu.SMEM((8, 128), jnp.int32),
            pltpu.VMEM((local_tiles, 2, lanes, pixels), jnp.int32),
            pltpu.VMEM((local_tiles, 4, lanes, pixels), jnp.float32),
            pltpu.VMEM((local_tiles, lanes, pixels), jnp.float32),
            pltpu.VMEM((2 * POINTS * PACK, pixels), jnp.float32),
            pltpu.VMEM((POINTS, tile_span, pixels), jnp.bfloat16),
            *[pltpu.VMEM((local_tiles * head_count * per_block, span, pixels), jnp.bfloat16) for span in spans],
            pltpu.VMEM((channels, depth), jnp.bfloat16),
            pltpu.VMEM((local_tiles, PACK, depth), jnp.bfloat16),
            pltpu.VMEM((head_count, local_tiles * head_dim, pixels), jnp.float32),
            pltpu.VMEM((head_count, local_tiles * head_dim, pixels), jnp.bfloat16),
            pltpu.VMEM((head_count, local_tiles * head_dim, pixels), jnp.bfloat16),
            dma((rows,)), dma((rows,)),
            dma((cols, parts)), dma((cols, parts)), dma((cols, parts)), dma((cols, parts)),
            dma((cols, rows, LEVELS)), dma((cols, rows, LEVELS)),
            dma((head_count,)), dma((head_count,)), dma((rows,)), dma((rows,)),
            dma((cols,)), dma((cols,)), dma((cols,)), dma((cols,)), dma, dma((13,)),
        ],
        compiler_params=pltpu.CompilerParams(
            collective_id=1, has_side_effects=True, vmem_limit_bytes=44 * 1024 * 1024
        ),
        name="fused",
    )(*[pltpu.with_memory_space_constraint(one, pltpu.HBM) for one in (*flat, *held)])


def on_device(
    queries,
    level_zero,
    level_one,
    level_two,
    level_three,
    tile_lists,
    samples,
    logit_weight,
    logit_bias,
    output_weight,
    output_bias,
    norm_gain,
    norm_shift,
):
    level_blocks = (level_zero, level_one, level_two, level_three)
    tile_rows, tile_cols, level_count, per_block = tile_lists.shape
    local_tiles = tile_rows * tile_cols
    requests = local_tiles * per_block
    channels = level_zero.shape[2]
    width_all = queries.shape[2]
    tile_side = level_zero.shape[0] // tile_rows
    pixels = tile_side * tile_side
    sides = [level.shape[0] // tile_rows for level in level_blocks]
    spans = [max(PACK, side * side) for side in sides]
    peer_count = lax.axis_size("row") * lax.axis_size("col")
    full = requests == 2 * peer_count and tile_cols == 1 and sides == [16, 8, 4, 2]
    full = full and all(power_of_two(n) for n in (tile_rows, lax.axis_size("col"), per_block))
    full = full and lax.axis_size("head") == 2 and width_all == 2 * channels
    if full:
        updated = fused_layer(
            queries, level_blocks, tile_lists, samples, logit_weight, logit_bias, output_weight,
            output_bias, norm_gain, norm_shift, sides, spans
        )
        return updated.reshape(tile_rows * tile_side, tile_cols * tile_side, channels)
    attn_out = gathered_attention(
        queries, level_blocks, tile_lists, samples, logit_weight, logit_bias, sides, spans
    )
    queries_blocked = to_blocks(queries, tile_rows, tile_cols, tile_side)

    head_index = lax.axis_index("head")
    full_attn = lax.all_gather(attn_out, "head", axis=1, tiled=True)
    pre_norm = (
        queries_blocked.reshape(local_tiles * pixels, width_all).astype(jnp.float32)
        + jnp.dot(full_attn, output_weight, preferred_element_type=jnp.float32)
        + output_bias
    )
    row_mean = jnp.mean(pre_norm, axis=1, keepdims=True)
    centered = pre_norm - row_mean
    variance = jnp.mean(centered * centered, axis=1, keepdims=True)
    own_part = lax.dynamic_slice_in_dim(centered, head_index * channels, channels, 1)
    normalized = own_part * lax.rsqrt(variance + 1e-05)
    updated = (normalized * norm_gain + norm_shift).astype(jnp.bfloat16)
    updated = updated.reshape(tile_rows, tile_cols, tile_side, tile_side, channels).transpose(
        0, 2, 1, 3, 4
    )
    return updated.reshape(tile_rows * tile_side, tile_cols * tile_side, channels)


def solution(mesh):
    in_specs = (
        P("row", "col", None),
        P("row", "col", "head"),
        P("row", "col", "head"),
        P("row", "col", "head"),
        P("row", "col", "head"),
        P("row", "col", None, None),
        P("row", "col", "head"),
        P(None, "head"),
        P("head"),
        P(),
        P(),
        P("head"),
        P("head"),
    )
    out_specs = P("row", "col", "head")
    return jax.shard_map(
        on_device, mesh=mesh, in_specs=in_specs, out_specs=out_specs, check_vma=False
    )
```
